32 devices in a mesh: wide: 16 (over z, y, x), narrow: 2 (over core).
Axes of the slice: x: 2, y: 2, z: 4, core: 2. Of those that a mesh axis runs over, the one named last changes fastest.
Arguments:
- tokens: bfloat16 [4096, 4096], P(('wide', 'narrow')), may hold values from -6 to 6
- expert_ids: int32 [4096, 2], P(('wide', 'narrow')), may hold values from 0 to 31, all different within a row; in each aligned block of 128 rows (0 to 127, 128 to 255, ...) at most 12 rows name the same one
- gate_values: bfloat16 [4096, 2], P(('wide', 'narrow')), may hold values from 0.099609375 to 1
- capacity: int32 [32], replicated, may hold values from 128 to 383
- w_gate: bfloat16 [32, 4096, 768], P(('wide', 'narrow')), may hold values from -0.09375 to 0.09375
- w_up: bfloat16 [32, 4096, 768], P(('wide', 'narrow')), may hold values from -0.09375 to 0.09375
- w_down: bfloat16 [32, 768, 4096], P(('wide', 'narrow')), may hold values from -0.21875 to 0.21875
Outputs:
- mixed: bfloat16 [4096, 4096], P(('wide', 'narrow'))
The draws below stay inside these ranges and needn't reach their ends.
Inputs may be any that keep to these rules, and one draw needn't show every extreme that they name: `expert_ids`: the two experts of a token differ; among the tokens of one device no expert is named more than 12 times, and that many is reached.
All inputs are finite; a program needn't handle non-finite values.
Results may differ from the reference program's by a relative error of at most 0.0058.
Values may be sent and summed in bfloat16 or wider, within the bound.
A program may use at most 128 MiB of HBM per device.

```python
import math
import jax
import jax.numpy as jnp
import numpy as np
from jax import lax

D = 4096
FF = 768
TOK_DEV = 128
TOKENS = 4096
EXPERTS = 32
MOST = 12


def with_ends(array, rng, least, largest):
    dims = array.shape
    place = [jax.random.randint(jax.random.fold_in(rng, axis), (), 0, dims[axis]) for axis in range(len(dims))]
    array = array.at[tuple(place)].set(least)
    longest = dims.index(max(dims))
    place[longest] = (place[longest] + 1) % dims[longest]
    return array.at[tuple(place)].set(largest)


def block_levels(stream_key, dims, pieces, low, high):
    factor_of = 1.0
    for dim, blocks in pieces:
        heights = jax.random.uniform(jax.random.fold_in(jax.random.fold_in(stream_key, 6), dim), (blocks,), jnp.float32, low / len(pieces), high / len(pieces))
        factor_of = factor_of * jnp.repeat(jnp.exp(heights), dims[dim] // blocks).reshape((-1,) + (1,) * (len(dims) - 1 - dim))
    return factor_of


def deal_out(own_key, own, number, rows, amount, top, bound, slope):
    order = jax.random.permutation(own_key, amount)
    packed, common = load_shares(amount, rows * top, bound, slope, True), load_shares(amount, rows * top, bound, slope, False)
    places = jnp.arange(amount)

    def named(tallies, turn):
        used = int((tallies > 0).sum())
        fixed = max(1, used // 4)
        passed = fixed + (places - fixed + turn * (used - fixed)) % max(1, amount - fixed)
        return jnp.zeros((amount,), jnp.int32).at[order[jnp.where(places < fixed, places, passed)]].set(jnp.asarray(tallies, jnp.int32))

    tallies = jnp.where(number % 4 == 0, named(packed, number // 4), named(common, number - number // 4 - 1))
    mixed = jax.random.permutation(jax.random.fold_in(own, 3), amount)
    donor, taker = mixed[0:amount // 2 * 2:2], mixed[1:amount // 2 * 2:2]
    slack = jnp.minimum(tallies[donor] - 1, bound - tallies[taker]) // 2
    slack = jnp.where((donor == order[0]) | (taker == order[0]) | (tallies[taker] == 0), 0, jnp.maximum(slack, 0))
    passed = jax.random.randint(jax.random.fold_in(own, 4), (amount // 2,), 0, 1 << 20) % (slack + 1)
    tallies = tallies.at[donor].add(-passed).at[taker].add(passed)
    labels = jnp.searchsorted(jnp.cumsum(tallies), jnp.arange(rows * top), side="right").astype(jnp.int32)
    listing = labels.reshape(top, rows).T
    listing = listing[jax.random.permutation(jax.random.fold_in(own, 1), rows)]
    turn = jax.random.randint(jax.random.fold_in(own, 2), (rows, 1), 0, top)
    return jnp.take_along_axis(listing, (jnp.arange(top)[None, :] + turn) % top, axis=1)


def load_shares(amount, total, reach, skew, full):
    loads = [(1 << 20) // math.isqrt(standing ** skew) + 1 for standing in range(1, amount + 1)]
    largest = reach if full else min(reach, max(-(-total // amount), total * loads[0] // sum(loads)))
    least = 1 if total - largest >= amount - 1 else 0
    counts, rest = [largest] + [least] * (amount - 1), total - largest - least * (amount - 1)
    while rest > 0:
        candidates = [i for i in range(1, amount) if counts[i] < largest] or [i for i in range(1, amount) if counts[i] < reach]
        whole, remaining = sum([loads[i] for i in candidates]), rest
        for i in candidates:
            addition = min(reach - counts[i], max(1, remaining * loads[i] // whole), rest)
            counts[i] = counts[i] + addition
            rest = rest - addition
    return np.array(counts)


def normal_values(key, extent, scale, limit, shards=(), kind=jnp.bfloat16):
    array = jax.random.normal(key, extent, jnp.float32) * scale
    if len(shards) > 0:
        array = block_levels(key, extent, shards, -0.22, 0.18) * array
    return jnp.clip(array, min=-limit, max=limit).astype(kind)


def setup_inputs(seed: int = 0) -> dict:
    splits = jax.random.split(jax.random.key(seed), 8)
    tokens = normal_values(splits[0], (TOKENS, D), 1.0, 6.0, ((0, 32),))
    expert_ids_keys = jax.random.split(jax.random.fold_in(splits[1], 1), TOKENS // TOK_DEV)
    expert_ids_turns = jax.random.permutation(jax.random.fold_in(splits[1], 3), TOKENS // TOK_DEV)
    expert_ids = jax.vmap(lambda own, number: deal_out(jax.random.fold_in(splits[1], 2), own, number, TOK_DEV, EXPERTS, 2, MOST, 2))(expert_ids_keys, expert_ids_turns).reshape((TOKENS, 2))
    gate_values = jnp.clip(0.099609375 + 0.9003906 * jax.random.uniform(splits[2], (TOKENS, 2), jnp.float32) ** block_levels(splits[2], (TOKENS, 2), ((0, 32),), -0.2, 0.2), 0.099609375, 1.0).astype(jnp.bfloat16)
    capacity = with_ends(jax.random.randint(splits[3], (EXPERTS,), TOK_DEV, 3 * TOK_DEV), jax.random.fold_in(splits[3], 1), TOK_DEV, (3 * TOK_DEV) - 1).astype(jnp.int32)
    w_gate = normal_values(splits[4], (EXPERTS, D, FF), D ** -0.5, 0.09375, ((0, 32),))
    w_up = normal_values(splits[5], (EXPERTS, D, FF), D ** -0.5, 0.09375, ((0, 32),))
    w_down = normal_values(splits[6], (EXPERTS, FF, D), FF ** -0.5, 0.21875, ((0, 32),))
    return {"tokens": tokens, "expert_ids": expert_ids, "gate_values": gate_values, "capacity": capacity, "w_gate": w_gate, "w_up": w_up, "w_down": w_down}


def expert_apply(token_rows, gate_matrix, up_matrix, down_matrix):
    gate_part = jnp.dot(token_rows, gate_matrix, preferred_element_type=jnp.float32)
    up_part = jnp.dot(token_rows, up_matrix, preferred_element_type=jnp.float32)
    hidden = (jax.nn.silu(gate_part) * up_part).astype(jnp.bfloat16)
    return jnp.dot(hidden, down_matrix, preferred_element_type=jnp.float32).astype(jnp.bfloat16)


def reference(tokens, expert_ids, gate_values, capacity, w_gate, w_up, w_down):
    assigns = 2 * TOKENS
    flat_ids = expert_ids.reshape(-1).astype(jnp.int32)
    onehot = (flat_ids[:, None] == jnp.arange(EXPERTS, dtype=jnp.int32)[None, :]).astype(jnp.int32)
    global_rank = jnp.sum((jnp.cumsum(onehot, axis=0) - onehot) * onehot, axis=1).astype(jnp.int32)
    kept_mask = global_rank < capacity[flat_ids]
    room_rows = 3 * TOK_DEV
    slot_index = jnp.where(kept_mask, global_rank, room_rows).astype(jnp.int32)
    table = jnp.full((EXPERTS, room_rows + 1), assigns, jnp.int32)
    table = table.at[flat_ids, slot_index].set(jnp.arange(assigns, dtype=jnp.int32))
    table = table[:, :room_rows]
    weights = gate_values.reshape(-1).astype(jnp.float32) * kept_mask.astype(jnp.float32)
    padded_weights = jnp.concatenate([weights, jnp.zeros((1,), jnp.float32)])
    padded_tokens = jnp.concatenate([tokens, jnp.zeros((1, D), jnp.bfloat16)], axis=0)

    def expert_step(summed, inputs):
        column, gate_matrix, up_matrix, down_matrix = inputs
        owners = (column // 2).astype(jnp.int32)
        token_rows = padded_tokens[owners]
        results = expert_apply(token_rows, gate_matrix, up_matrix, down_matrix)
        scaled = results.astype(jnp.float32) * padded_weights[column][:, None]
        return summed.at[owners].add(scaled), None

    start = jnp.zeros((TOKENS + 1, D), jnp.float32)
    summed, unused = lax.scan(expert_step, start, (table, w_gate, w_up, w_down))
    return summed[:TOKENS].astype(jnp.bfloat16)
```

```python
import functools
import math

import jax
import jax.numpy as jnp
import numpy as np
from jax import lax
from jax.experimental import pallas as pl
from jax.experimental.pallas import tpu as pltpu
from jax.sharding import PartitionSpec as P

MESH = pl.DeviceIdType.MESH
PIECES = 16
PLANES = 4
F32 = jnp.float32
BF16 = jnp.bfloat16
NT = (((1,), (1,)), ((), ()))


def flip(me, off, bits):
    out = 0
    for b in range(bits):
        w = 1 << b
        out = out + (((me // w) % 2 + (off // w) % 2) % 2) * w
    return out


def kernel(n, narrow, most, unit, tok, ids, gates, cap, code, turn, lane, gather, spread,
           wg_hbm, wu_hbm, wd_hbm, out,
           wg, wu, wd, sent, came, back, home, far, mixed, cross, x, h, total, note, meta, cnt, seen, left,
           s_sent, r_came, s_back, r_home, s_far, r_far, s_mixed, r_cross, s_note, r_note, s_cnt, r_cnt, wsem):
    bits = int(math.log2(n))
    half, plane = n // 2, n // PLANES
    rows, part = unit * unit * most, unit * most
    tok_rows, width = tok.shape
    hidden = wg.shape[1]
    lanes = cnt.shape[1]
    piece = width // PIECES
    quads = PIECES // unit
    wide_cols = unit * piece
    me = lax.axis_index("wide") * narrow + lax.axis_index("narrow")
    place = me // plane
    inner = jnp.logical_or(place == 1, place == 2)
    is_inner = jnp.where(inner, 1, 0)
    relay_off = (2 + is_inner) * plane
    which = 1 - is_inner

    def where_is(off):
        peer = flip(me, off, bits)
        return (peer // narrow, peer % narrow)

    def remote(src, dst, send, recv, off):
        return pltpu.make_async_remote_copy(
            src_ref=src, dst_ref=dst, send_sem=send, recv_sem=recv,
            device_id=where_is(off), device_id_type=MESH)

    def groups(count, body):
        if unit <= 4:
            for g in range(count):
                body(g)
        else:
            pl.loop(0, count)(body)

    def columns(q, j):
        return pl.ds(pl.multiple_of((q * unit + j) * piece, piece), piece)

    def quad_columns(q):
        return pl.ds(pl.multiple_of(q * wide_cols, wide_cols), wide_cols)

    def quad_rows(q):
        return pl.ds(pl.multiple_of(q * part, part), part)

    loads = [
        pltpu.make_async_copy(hbm.at[0], v, wsem.at[i])
        for i, (hbm, v) in enumerate(((wg_hbm, wg), (wu_hbm, wu), (wd_hbm, wd)))
    ]
    for load in loads:
        load.start()

    barrier = pltpu.get_barrier_semaphore()

    @pl.loop(1, n)
    def _(off):
        pl.semaphore_signal(barrier, inc=1, device_id=where_is(off), device_id_type=MESH)

    names = [ids[c:c + 1, :] for c in (0, 1)]
    expert = lax.broadcasted_iota(jnp.int32, (lanes, tok_rows), 0)
    hot = [jnp.where(expert == name, 1.0, 0.0) for name in names]
    both = (hot[0] + hot[1]).astype(BF16)
    ahead = lax.broadcasted_iota(jnp.int32, (tok_rows, tok_rows), 0) < lax.broadcasted_iota(
        jnp.int32, (tok_rows, tok_rows), 1)
    before = jnp.dot(both, jnp.where(ahead, 1.0, 0.0).astype(BF16), preferred_element_type=F32)
    ranks = [jnp.sum(o * before, axis=0, keepdims=True) for o in hot]
    tally = lax.dot_general(jnp.ones((8, tok_rows), BF16), both, NT, preferred_element_type=F32)
    cnt[...] = tally[0:1, :]
    seen[0] = tally[0:1, :]
    relay = flip(me, relay_off, bits)
    for host, ref in ((me, meta.at[0]), (relay, note)):
        slots = [((name ^ host) * most).astype(F32) + rank for name, rank in zip(names, ranks)]
        ref[0:1, :] = slots[0]
        ref[1:2, :] = slots[1]
        ref[2:4, :] = gates[...]

    pl.semaphore_wait(barrier, n - 1)

    note_copy = remote(note, meta.at[1 + which], s_note, r_note.at[which], relay_off)
    note_copy.start()

    @pl.loop(1, n)
    def _(off):
        remote(cnt, seen.at[off], s_cnt, r_cnt, off).start()

    def far_copy(q):
        return remote(tok.at[:, quad_columns(q)], far.at[which, :, quad_columns(q)],
                      s_far, r_far.at[which, q], relay_off)

    def send_far():
        @pl.loop(0, quads)
        def _(q):
            far_copy(q).start()

    def pack(k, q):
        slots = [meta[k, c:c + 1, :] for c in (0, 1)]
        base = 0 if k == 0 else half + (k - 1) * plane

        def group(g):
            acc = jnp.zeros((rows, piece), F32)
            for j in range(unit):
                mine = jnp.where(turn[...] == j, code[...] + jnp.asarray(g * part, F32), -1.0)
                hit = jnp.where(mine == slots[0], 1.0, 0.0) + jnp.where(mine == slots[1], 1.0, 0.0)
                put = hit.astype(BF16)
                values = tok[:, columns(q, j)] if k == 0 else far[k - 1, :, columns(q, j)]
                acc = acc + jnp.dot(put, values, preferred_element_type=F32)
            sent[pl.ds(k * half + g * unit, unit), quad_rows(q), :] = acc.astype(BF16).reshape(unit, part, piece)

        groups(half // unit, group)

        @pl.loop(1, half)
        def _(off):
            into = base + off if k == 0 else base + off % plane
            remote(sent.at[k * half + off, quad_rows(q), :], came.at[into, quad_rows(q), :],
                   s_sent.at[k], r_came.at[k, q], off).start()

        came[base, quad_rows(q), :] = sent[k * half, quad_rows(q), :]

    def pack_far(k, q):
        remote(tok.at[:, quad_columns(q)], far.at[k - 1, :, quad_columns(q)],
               s_far, r_far.at[k - 1, q], relay_off).wait_recv()
        pack(k, q)

    def block_copy(ref, first, last, q, send, recv):
        piece_of = ref.at[pl.ds(first, last - first), quad_rows(q), :]
        return remote(piece_of, piece_of, send, recv, relay_off)

    def expert_rows(k):
        base = 0 if k == 0 else half + (k - 1) * plane
        blocks = half if k == 0 else plane
        count = blocks * most

        @pl.loop(0, quads)
        def _(q):
            if k == 0:
                block_copy(came, 1, half, q, s_back.at[k], r_came.at[k, q]).wait_recv()
            else:
                @pl.when(inner)
                def _():
                    block_copy(came, base + 1, base + plane, q, s_back.at[k], r_came.at[k, q]).wait_recv()

                @pl.when(jnp.logical_not(inner))
                def _():
                    block_copy(came, base, base + plane, q, s_back.at[k], r_came.at[k, q]).wait_recv()

            def group(g):
                block = came[pl.ds(base + g * unit, unit), quad_rows(q), :].reshape(rows, piece)
                for j in range(unit):
                    x[pl.ds(g * part, part), columns(q, j)] = jnp.dot(
                        gather[j], block, preferred_element_type=F32).astype(BF16)

            groups(blocks // unit, group)

        step = math.gcd(hidden, 256)

        @pl.loop(0, hidden // step)
        def _(t):
            at = pl.ds(pl.multiple_of(t * step, step), step)
            gate = jnp.dot(x[0:count, :], wg[:, at], preferred_element_type=F32)
            up = jnp.dot(x[0:count, :], wu[:, at], preferred_element_type=F32)
            h[0:count, at] = (gate / (1.0 + jnp.exp(-gate)) * up).astype(BF16)

        @pl.loop(0, quads)
        def _(q):
            for j in range(unit):
                x[0:count, j * piece:(j + 1) * piece] = jnp.dot(
                    h[0:count, :], wd[:, columns(q, j)], preferred_element_type=F32).astype(BF16)

            def group(g):
                acc = jnp.zeros((rows, piece), F32)
                for j in range(unit):
                    acc = acc + jnp.dot(spread[j], x[pl.ds(g * part, part), j * piece:(j + 1) * piece],
                                        preferred_element_type=F32)
                back[pl.ds(base + g * unit, unit), quad_rows(q), :] = acc.astype(BF16).reshape(unit, part, piece)

            groups(blocks // unit, group)

            if k == 0:
                @pl.loop(1, half)
                def _(off):
                    remote(back.at[off, quad_rows(q), :], home.at[off, quad_rows(q), :],
                           s_back.at[k], r_home.at[k, q], off).start()

                home[0, quad_rows(q), :] = back[0, quad_rows(q), :]
            else:
                def reply(low):
                    off = low + (1 - is_inner) * plane
                    remote(back.at[base + low, quad_rows(q), :], home.at[k * half + off, quad_rows(q), :],
                           s_back.at[k], r_home.at[k, q], off).start()

                @pl.when(jnp.logical_not(inner))
                def _():
                    reply(0)

                @pl.loop(1, plane)
                def _(low):
                    reply(low)

                @pl.when(inner)
                def _():
                    home[k * half, quad_rows(q), :] = back[base, quad_rows(q), :]

    def room_for(source):
        def earlier(off, sums):
            return sums + seen[off] * jnp.where(flip(me, off, bits) < source, 1.0, 0.0)

        sums = lax.fori_loop(0, n, earlier, jnp.zeros((1, lanes), F32))
        return jnp.broadcast_to(jnp.clip(cap[...] - sums, 0.0, float(most)), (8, lanes))

    def rooms():
        remote(seen.at[pl.ds(1, n - 1)], seen.at[pl.ds(1, n - 1)], s_cnt, r_cnt, relay_off).wait_recv()
        left[0] = room_for(me)

        @pl.when(inner)
        def _():
            left[1] = room_for(flip(me, 3 * plane, bits))
            left[2] = room_for(flip(me, 2 * plane, bits))

    def combine(k, q):
        slots = [meta[k, c:c + 1, :] for c in (0, 1)]
        shares = [meta[k, c:c + 1, :] for c in (2, 3)]
        room_of = left[k].astype(BF16)
        eye = jnp.where(
            lax.broadcasted_iota(jnp.int32, (tok_rows, tok_rows), 0)
            == lax.broadcasted_iota(jnp.int32, (tok_rows, tok_rows), 1), 1.0, 0.0).astype(BF16)
        block_copy(home, k * half + 1, (k + 1) * half, q, s_back.at[k], r_home.at[k, q]).wait_recv()
        total[...] = jnp.zeros_like(total)

        def group(g):
            mine = code[...] + jnp.asarray(g * part, F32)
            weight = (jnp.where(mine == slots[0], shares[0], 0.0)
                      + jnp.where(mine == slots[1], shares[1], 0.0)).astype(BF16)
            weight = lax.dot_general(eye, weight, NT, preferred_element_type=F32)
            owner = lax.broadcasted_iota(jnp.int32, (lanes, rows), 0)
            pick = jnp.where(owner == ((lane[0:1, :] + g * unit) ^ me), 1.0, 0.0).astype(BF16)
            room = jnp.dot(room_of, pick, preferred_element_type=F32)[0:1, :]
            weight = jnp.where(room > lane[2:3, :].astype(F32), weight, 0.0)
            block = home[pl.ds(k * half + g * unit, unit), quad_rows(q), :].reshape(rows, piece)
            for j in range(unit):
                masked = jnp.where(lane[1:2, :] == j, weight, 0.0).astype(BF16)
                total[:, j * piece:(j + 1) * piece] += jnp.dot(masked, block, preferred_element_type=F32)

        groups(half // unit, group)

    def combine_far(k):
        @pl.loop(0, quads)
        def _(q):
            combine(k, q)
            mixed[k - 1, :, quad_columns(q)] = total[...].astype(BF16)
            at = quad_columns(q)
            remote(mixed.at[k - 1, :, at], cross.at[:, at], s_mixed.at[k - 1], r_cross.at[q],
                   (4 - k) * plane).start()

    @pl.when(inner)
    def _():
        send_far()

    @pl.loop(0, quads)
    def _(q):
        pack(0, q)

    @pl.when(jnp.logical_not(inner))
    def _():
        send_far()

    @pl.when(inner)
    def _():
        for k in (1, 2):
            remote(note, meta.at[k], s_note, r_note.at[k - 1], relay_off).wait_recv()

        @pl.loop(0, quads)
        def _(q):
            pack_far(1, q)

    for load in loads:
        load.wait()

    expert_rows(0)

    @pl.when(inner)
    def _():
        @pl.loop(0, quads)
        def _(q):
            pack_far(2, q)

    expert_rows(1)
    rooms()

    @pl.when(inner)
    def _():
        combine_far(1)

    expert_rows(2)

    @pl.when(inner)
    def _():
        combine_far(2)

    @pl.loop(0, quads)
    def _(q):
        combine(0, q)
        at = quad_columns(q)
        remote(cross.at[:, at], cross.at[:, at], s_far, r_cross.at[q], relay_off).wait_recv()
        out[:, at] = (total[...] + cross[:, at].astype(F32)).astype(BF16)

    note_copy.wait_send()
    remote(seen.at[pl.ds(1, n - 1)], seen.at[pl.ds(1, n - 1)], s_cnt, r_cnt, relay_off).wait_send()
    remote(tok, cross, s_far, r_far.at[0, 0], relay_off).wait_send()

    def sent_all(ref, first, last, send):
        some = ref.at[pl.ds(first, last - first)]
        remote(some, some, send, r_cnt, relay_off).wait_send()

    sent_all(sent, 1, half, s_sent.at[0])
    sent_all(back, 1, half, s_back.at[0])

    @pl.when(inner)
    def _():
        for k in (1, 2):
            base = half + (k - 1) * plane
            sent_all(sent, k * half + 1, (k + 1) * half, s_sent.at[k])
            sent_all(back, base + 1, base + plane, s_back.at[k])
            remote(mixed.at[k - 1], cross, s_mixed.at[k - 1], r_cnt, relay_off).wait_send()

    @pl.when(jnp.logical_not(inner))
    def _():
        for k in (1, 2):
            base = half + (k - 1) * plane
            sent_all(back, base, base + plane, s_back.at[k])


def on_device(n, narrow, tokens, expert_ids, gate_values, capacity, w_gate, w_up, w_down):
    experts = capacity.shape[0]
    tok_rows, width = tokens.shape
    hidden = w_gate.shape[2]
    most = 3 * tok_rows // experts
    unit = 16 // math.gcd(16, most)
    half, plane = n // 2, n // PLANES
    rows = unit * unit * most
    quads = PIECES // unit
    lanes = -(-experts // 128) * 128

    i, j, r = np.meshgrid(np.arange(unit), np.arange(unit), np.arange(most), indexing="ij")
    i, j, r = i.reshape(-1), j.reshape(-1), r.reshape(-1)
    code = jnp.asarray(np.broadcast_to((i * most + r)[:, None], (rows, tok_rows)), F32)
    turn = jnp.asarray(np.broadcast_to(j[:, None], (rows, tok_rows)), F32)
    lane = jnp.asarray(np.stack([i, j, r] + [0 * r] * 5), jnp.int32)
    short = np.arange(unit * most)
    every = np.arange(unit)
    gather = (short[None, :, None] == (i * most + r)[None, None, :]) & (j[None] == every[:, None])[:, None, :]
    gather, spread = jnp.asarray(gather, BF16), jnp.asarray(gather.transpose(0, 2, 1), BF16)
    cap = jnp.pad(capacity, (0, lanes - experts))[None].astype(F32)

    block = (PIECES * most, width // PIECES)
    vmem = pl.BlockSpec(memory_space=pltpu.VMEM)
    hbm = pl.BlockSpec(memory_space=pl.ANY)
    dma = pltpu.SemaphoreType.DMA
    return pl.pallas_call(
        functools.partial(kernel, n, narrow, most, unit),
        out_shape=jax.ShapeDtypeStruct((tok_rows, width), BF16),
        in_specs=[vmem] * 9 + [hbm] * 3,
        out_specs=vmem,
        scratch_shapes=[
            pltpu.VMEM((width, hidden), BF16),
            pltpu.VMEM((width, hidden), BF16),
            pltpu.VMEM((hidden, width), BF16),
            pltpu.VMEM((3 * half,) + block, BF16),
            pltpu.VMEM((half + 2 * plane,) + block, BF16),
            pltpu.VMEM((half + 2 * plane,) + block, BF16),
            pltpu.VMEM((3 * half,) + block, BF16),
            pltpu.VMEM((2, tok_rows, width), BF16),
            pltpu.VMEM((2, tok_rows, width), BF16),
            pltpu.VMEM((tok_rows, width), BF16),
            pltpu.VMEM((half * most, width), BF16),
            pltpu.VMEM((half * most, hidden), BF16),
            pltpu.VMEM((tok_rows, unit * width // PIECES), F32),
            pltpu.VMEM((8, tok_rows), F32),
            pltpu.VMEM((3, 8, tok_rows), F32),
            pltpu.VMEM((1, lanes), F32),
            pltpu.VMEM((n, 1, lanes), F32),
            pltpu.VMEM((3, 8, lanes), F32),
            dma((3,)), dma((3, quads)), dma((3,)), dma((3, quads)), dma, dma((2, quads)), dma((2,)),
            dma((quads,)), dma, dma((2,)), dma, dma, dma((3,)),
        ],
        compiler_params=pltpu.CompilerParams(
            collective_id=0, has_side_effects=True, vmem_limit_bytes=60 * 1024 * 1024
        ),
    )(tokens, expert_ids.T, gate_values.T.astype(F32), cap, code, turn, lane, gather, spread, w_gate, w_up, w_down)


def solution(mesh):
    both = ("wide", "narrow")
    n, narrow = mesh.shape["wide"] * mesh.shape["narrow"], mesh.shape["narrow"]
    return jax.shard_map(
        functools.partial(on_device, n, narrow),
        mesh=mesh,
        in_specs=(P(both, None), P(both, None), P(both, None), P(),
                  P(both, None, None), P(both, None, None), P(both, None, None)),
        out_specs=P(both, None),
        check_vma=False,
    )
```

```python
import functools
import math

import jax
import jax.numpy as jnp
import numpy as np
from jax import lax
from jax.experimental import pallas as pl
from jax.experimental.pallas import tpu as pltpu
from jax.sharding import PartitionSpec as P

MESH = pl.DeviceIdType.MESH
PIECES = 16
PLANES = 4
F32 = jnp.float32
BF16 = jnp.bfloat16
NT = (((1,), (1,)), ((), ()))


def flip(me, off, bits):
    out = 0
    for b in range(bits):
        w = 1 << b
        out = out + (((me // w) % 2 + (off // w) % 2) % 2) * w
    return out


def kernel(n, narrow, most, unit, ids, gates, cap, lane, tok_hbm, code_hbm, turn_hbm, gather_hbm, spread_hbm,
           wg_hbm, wu_hbm, wd_hbm, out_hbm,
           tok, code, turn, gather, spread, wg, wu, wd, out,
           sent, came, back, home, far, mixed, cross, x, h, h_own, total, note, meta, cnt, seen, left,
           s_sent, r_came, s_back, r_home, s_far, r_far, s_mixed, r_cross, s_note, r_note, s_cnt, r_cnt,
           lsem, wsem, osem):
    bits = int(math.log2(n))
    half, plane = n // 2, n // PLANES
    rows, part = unit * unit * most, unit * most
    tok_rows, width = tok.shape
    hidden = wg.shape[1]
    lanes = cnt.shape[1]
    piece = width // PIECES
    quads = PIECES // unit
    wide_cols = unit * piece
    me = lax.axis_index("wide") * narrow + lax.axis_index("narrow")
    place = me // plane
    inner = jnp.logical_or(place == 1, place == 2)
    is_inner = jnp.where(inner, 1, 0)
    relay_off = (2 + is_inner) * plane
    which = 1 - is_inner

    mine = [((me // (1 << b)) % 2) * (1 << b) for b in range(bits)]
    level = int(math.log2(plane))
    facing = list(mine)
    facing[level] = jnp.where(inner, mine[level], plane - mine[level])

    def where_is(off, origin=mine):
        if isinstance(off, int):
            peer = [(1 << b) - v if (off >> b) % 2 else v for b, v in enumerate(origin)]
            low = int(math.log2(narrow))
            return (sum(peer[low:]) // narrow, sum(peer[:low]))
        peer = flip(sum(origin), off, bits)
        return (peer // narrow, peer % narrow)

    def remote(src, dst, send, recv, off, origin=mine):
        return pltpu.make_async_remote_copy(
            src_ref=src, dst_ref=dst, send_sem=send, recv_sem=recv,
            device_id=where_is(off, origin), device_id_type=MESH)

    def each(first, last, body):
        if last - first <= 32:
            for off in range(first, last):
                body(off)
        else:
            pl.loop(first, last)(body)

    def groups(count, body):
        if unit <= 4:
            for g in range(count):
                body(g)
        else:
            pl.loop(0, count)(body)

    def columns(q, j):
        return pl.ds(pl.multiple_of((q * unit + j) * piece, piece), piece)

    def quad_columns(q):
        return pl.ds(pl.multiple_of(q * wide_cols, wide_cols), wide_cols)

    def quad_rows(q):
        return pl.ds(pl.multiple_of(q * part, part), part)

    barrier = pltpu.get_barrier_semaphore()

    with jax.named_scope("signals"):
        each(1, n, lambda off: pl.semaphore_signal(
            barrier, inc=1, device_id=where_is(off), device_id_type=MESH))

    inputs = [
        pltpu.make_async_copy(hbm, v, lsem.at[i])
        for i, (hbm, v) in enumerate(((tok_hbm, tok), (code_hbm, code), (turn_hbm, turn),
                                      (gather_hbm, gather), (spread_hbm, spread)))
    ]
    loads = [
        pltpu.make_async_copy(hbm.at[0], v, wsem.at[i])
        for i, (hbm, v) in enumerate(((wg_hbm, wg), (wu_hbm, wu), (wd_hbm, wd)))
    ]
    for load in inputs:
        load.start()

    names = [ids[c:c + 1, :] for c in (0, 1)]
    expert = lax.broadcasted_iota(jnp.int32, (lanes, tok_rows), 0)
    hot = [jnp.where(expert == name, 1.0, 0.0) for name in names]
    both = (hot[0] + hot[1]).astype(BF16)
    ahead = lax.broadcasted_iota(jnp.int32, (tok_rows, tok_rows), 0) < lax.broadcasted_iota(
        jnp.int32, (tok_rows, tok_rows), 1)
    before = jnp.dot(both, jnp.where(ahead, 1.0, 0.0).astype(BF16), preferred_element_type=F32)
    ranks = [jnp.sum(o * before, axis=0, keepdims=True) for o in hot]
    tally = lax.dot_general(jnp.ones((8, tok_rows), BF16), both, NT, preferred_element_type=F32)
    cnt[...] = tally[0:1, :]
    left[0] = jnp.zeros((8, lanes), F32)
    left[0, 0:1, 0:cap.shape[1]] = cap[...].astype(F32)
    limit = left[0, 0:1, :]
    seen[0] = tally[0:1, :]
    relay = flip(me, relay_off, bits)
    for host, ref in ((me, meta.at[0]), (relay, note)):
        slots = [((name ^ host) * most).astype(F32) + rank for name, rank in zip(names, ranks)]
        ref[0:1, :] = slots[0]
        ref[1:2, :] = slots[1]
        ref[2:4, :] = gates[...].astype(F32)

    for load in inputs:
        load.wait()

    with jax.named_scope("barrier"):
        pl.semaphore_wait(barrier, n - 1)

    for load in loads:
        load.start()

    note_copy = remote(note, meta.at[1 + which], s_note, r_note.at[which], relay_off)
    note_copy.start()

    each(1, n, lambda off: remote(cnt, seen.at[off], s_cnt, r_cnt, off).start())

    def far_copy(q):
        return remote(tok.at[:, quad_columns(q)], far.at[which, :, quad_columns(q)],
                      s_far, r_far.at[which, q], relay_off)

    def send_far():
        @pl.loop(0, quads)
        def _(q):
            far_copy(q).start()

    def pack(k, q):
        slots = [meta[k, c:c + 1, :] for c in (0, 1)]
        base = 0 if k == 0 else half + (k - 1) * plane

        def group(g):
            acc = jnp.zeros((rows, piece), F32)
            for j in range(unit):
                mine = jnp.where(turn[...] == j, code[...] + jnp.asarray(g * part, F32), -1.0)
                hit = jnp.where(mine == slots[0], 1.0, 0.0) + jnp.where(mine == slots[1], 1.0, 0.0)
                put = hit.astype(BF16)
                values = tok[:, columns(q, j)] if k == 0 else far[k - 1, :, columns(q, j)]
                acc = acc + jnp.dot(put, values, preferred_element_type=F32)
            sent[pl.ds(k * half + g * unit, unit), quad_rows(q), :] = acc.astype(BF16).reshape(unit, part, piece)

        with jax.named_scope(f"pack{k}"):
            groups(half // unit, group)

        def deal(off):
            into = base + off if k == 0 else base + off % plane
            remote(sent.at[k * half + off, quad_rows(q), :], came.at[into, quad_rows(q), :],
                   s_sent.at[k], r_came.at[k, q], off).start()

        each(1, half, deal)

        came[base, quad_rows(q), :] = sent[k * half, quad_rows(q), :]

    def pack_far(k, q):
        with jax.named_scope(f"wait_far{k}"):
            remote(tok.at[:, quad_columns(q)], far.at[k - 1, :, quad_columns(q)],
                   s_far, r_far.at[k - 1, q], relay_off).wait_recv()
        pack(k, q)

    def block_copy(ref, first, last, q, send, recv):
        piece_of = ref.at[pl.ds(first, last - first), quad_rows(q), :]
        return remote(piece_of, piece_of, send, recv, relay_off)

    def receive(k):
        base = 0 if k == 0 else half + (k - 1) * plane
        blocks = half if k == 0 else plane

        @pl.loop(0, quads)
        def _(q):
            with jax.named_scope(f"wait_came{k}"):
                if k == 0:
                    block_copy(came, 1, half, q, s_back.at[k], r_came.at[k, q]).wait_recv()
                else:
                    @pl.when(inner)
                    def _():
                        block_copy(came, base + 1, base + plane, q, s_back.at[k], r_came.at[k, q]).wait_recv()

                    @pl.when(jnp.logical_not(inner))
                    def _():
                        block_copy(came, base, base + plane, q, s_back.at[k], r_came.at[k, q]).wait_recv()

            def group(g):
                block = came[pl.ds(base + g * unit, unit), quad_rows(q), :].reshape(rows, piece)
                for j in range(unit):
                    x[pl.ds(g * part, part), columns(q, j)] = jnp.dot(
                        gather[j], block, preferred_element_type=F32).astype(BF16)

            with jax.named_scope(f"unpack{k}"):
                groups(blocks // unit, group)

    def gate_up(k, h):
        count = (half if k == 0 else plane) * most
        step = math.gcd(hidden, 256)

        @pl.loop(0, hidden // step)
        def _(t):
            at = pl.ds(pl.multiple_of(t * step, step), step)
            with jax.named_scope(f"gate_up{k}"):
                gate = jnp.dot(x[0:count, :], wg[:, at], preferred_element_type=F32)
                up = jnp.dot(x[0:count, :], wu[:, at], preferred_element_type=F32)
                h[0:count, at] = (gate / (1.0 + jnp.exp(-gate)) * up).astype(BF16)

    def down(k, h):
        base = 0 if k == 0 else half + (k - 1) * plane
        blocks = half if k == 0 else plane
        count = blocks * most

        @pl.loop(0, quads)
        def _(q):
            with jax.named_scope(f"down{k}"):
                for j in range(unit):
                    x[0:count, j * piece:(j + 1) * piece] = jnp.dot(
                        h[0:count, :], wd[:, columns(q, j)], preferred_element_type=F32).astype(BF16)

            def group(g):
                acc = jnp.zeros((rows, piece), F32)
                for j in range(unit):
                    acc = acc + jnp.dot(spread[j], x[pl.ds(g * part, part), j * piece:(j + 1) * piece],
                                        preferred_element_type=F32)
                back[pl.ds(base + g * unit, unit), quad_rows(q), :] = acc.astype(BF16).reshape(unit, part, piece)

            with jax.named_scope(f"spread{k}"):
                groups(blocks // unit, group)

            if k == 0:
                def answer(off):
                    remote(back.at[off, quad_rows(q), :], home.at[off, quad_rows(q), :],
                           s_back.at[k], r_home.at[k, q], off).start()

                each(1, half, answer)
                home[0, quad_rows(q), :] = back[0, quad_rows(q), :]
            else:
                def reply(low):
                    off = low + (1 - is_inner) * plane
                    remote(back.at[base + low, quad_rows(q), :], home.at[k * half + off, quad_rows(q), :],
                           s_back.at[k], r_home.at[k, q], low, facing).start()

                @pl.when(jnp.logical_not(inner))
                def _():
                    reply(0)

                each(1, plane, reply)

                @pl.when(inner)
                def _():
                    home[k * half, quad_rows(q), :] = back[base, quad_rows(q), :]

    def room_for(source):
        def earlier(off, sums):
            return sums + seen[off] * jnp.where(flip(me, off, bits) < source, 1.0, 0.0)

        sums = lax.fori_loop(0, n, earlier, jnp.zeros((1, lanes), F32))
        return jnp.broadcast_to(jnp.clip(limit - sums, 0.0, float(most)), (8, lanes))

    def rooms():
        remote(seen.at[pl.ds(1, n - 1)], seen.at[pl.ds(1, n - 1)], s_cnt, r_cnt, relay_off).wait_recv()
        left[0] = room_for(me)

        @pl.when(inner)
        def _():
            left[1] = room_for(flip(me, 3 * plane, bits))
            left[2] = room_for(flip(me, 2 * plane, bits))

    def combine(k, q):
        slots = [meta[k, c:c + 1, :] for c in (0, 1)]
        shares = [meta[k, c:c + 1, :] for c in (2, 3)]
        room_of = left[k].astype(BF16)
        eye = jnp.where(
            lax.broadcasted_iota(jnp.int32, (tok_rows, tok_rows), 0)
            == lax.broadcasted_iota(jnp.int32, (tok_rows, tok_rows), 1), 1.0, 0.0).astype(BF16)
        with jax.named_scope(f"wait_home{k}"):
            block_copy(home, k * half + 1, (k + 1) * half, q, s_back.at[k], r_home.at[k, q]).wait_recv()
        total[...] = jnp.zeros_like(total)

        def group(g):
            mine = code[...] + jnp.asarray(g * part, F32)
            weight = (jnp.where(mine == slots[0], shares[0], 0.0)
                      + jnp.where(mine == slots[1], shares[1], 0.0)).astype(BF16)
            weight = lax.dot_general(eye, weight, NT, preferred_element_type=F32)
            owner = lax.broadcasted_iota(jnp.int32, (lanes, rows), 0)
            pick = jnp.where(owner == ((lane[0:1, :] + g * unit) ^ me), 1.0, 0.0).astype(BF16)
            room = jnp.dot(room_of, pick, preferred_element_type=F32)[0:1, :]
            weight = jnp.where(room > lane[2:3, :].astype(F32), weight, 0.0)
            block = home[pl.ds(k * half + g * unit, unit), quad_rows(q), :].reshape(rows, piece)
            for j in range(unit):
                masked = jnp.where(lane[1:2, :] == j, weight, 0.0).astype(BF16)
                total[:, j * piece:(j + 1) * piece] += jnp.dot(masked, block, preferred_element_type=F32)

        with jax.named_scope(f"combine{k}"):
            groups(half // unit, group)

    def combine_far(k, first, last):
        @pl.loop(first, last)
        def _(q):
            combine(k, q)
            mixed[k - 1, :, quad_columns(q)] = total[...].astype(BF16)
            at = quad_columns(q)
            remote(mixed.at[k - 1, :, at], cross.at[:, at], s_mixed.at[k - 1], r_cross.at[q],
                   (4 - k) * plane).start()

    def pack_own(first, last):
        @pl.loop(first, last)
        def _(q):
            pack(0, q)

    def relay_in(k, first, last):
        remote(note, meta.at[k], s_note, r_note.at[k - 1], relay_off).wait_recv()

        @pl.loop(first, last)
        def _(q):
            pack_far(k, q)

    @pl.when(jnp.logical_not(inner))
    def _():
        send_far()

    pack_own(0, quads // 2)

    @pl.when(inner)
    def _():
        send_far()
        relay_in(2, 0, quads)

    pack_own(quads // 2, quads)

    for load in loads:
        load.wait()

    receive(2)
    gate_up(2, h)
    down(2, h)

    @pl.when(inner)
    def _():
        relay_in(1, 0, quads)

    receive(0)
    gate_up(0, h_own)
    with jax.named_scope("rooms"):
        rooms()

    @pl.when(inner)
    def _():
        combine_far(2, 0, quads)

    receive(1)
    gate_up(1, h)
    down(1, h)
    down(0, h_own)

    @pl.when(inner)
    def _():
        combine_far(1, 0, quads)

    @pl.loop(0, quads)
    def _(q):
        combine(0, q)
        at = quad_columns(q)
        with jax.named_scope("wait_cross"):
            remote(cross.at[:, at], cross.at[:, at], s_far, r_cross.at[q], relay_off).wait_recv()
        out[:, at] = (total[...] + cross[:, at].astype(F32)).astype(BF16)
        pltpu.make_async_copy(out.at[:, at], out_hbm.at[:, at], osem.at[q]).start()

    @pl.loop(0, quads)
    def _(q):
        at = quad_columns(q)
        pltpu.make_async_copy(out.at[:, at], out_hbm.at[:, at], osem.at[q]).wait()

    note_copy.wait_send()
    remote(seen.at[pl.ds(1, n - 1)], seen.at[pl.ds(1, n - 1)], s_cnt, r_cnt, relay_off).wait_send()
    remote(tok, cross, s_far, r_far.at[0, 0], relay_off).wait_send()

    def sent_all(ref, first, last, send):
        some = ref.at[pl.ds(first, last - first)]
        remote(some, some, send, r_cnt, relay_off).wait_send()

    sent_all(sent, 1, half, s_sent.at[0])
    sent_all(back, 1, half, s_back.at[0])

    @pl.when(inner)
    def _():
        for k in (1, 2):
            base = half + (k - 1) * plane
            sent_all(sent, k * half + 1, (k + 1) * half, s_sent.at[k])
            sent_all(back, base + 1, base + plane, s_back.at[k])
            remote(mixed.at[k - 1], cross, s_mixed.at[k - 1], r_cnt, relay_off).wait_send()

    @pl.when(jnp.logical_not(inner))
    def _():
        for k in (1, 2):
            base = half + (k - 1) * plane
            sent_all(back, base, base + plane, s_back.at[k])


def on_device(n, narrow, tokens, expert_ids, gate_values, capacity, w_gate, w_up, w_down):
    experts = capacity.shape[0]
    tok_rows, width = tokens.shape
    hidden = w_gate.shape[2]
    most = 3 * tok_rows // experts
    unit = 16 // math.gcd(16, most)
    half, plane = n // 2, n // PLANES
    rows = unit * unit * most
    quads = PIECES // unit
    lanes = -(-experts // 128) * 128

    i, j, r = np.meshgrid(np.arange(unit), np.arange(unit), np.arange(most), indexing="ij")
    i, j, r = i.reshape(-1), j.reshape(-1), r.reshape(-1)
    code = jnp.asarray(np.broadcast_to((i * most + r)[:, None], (rows, tok_rows)), F32)
    turn = jnp.asarray(np.broadcast_to(j[:, None], (rows, tok_rows)), F32)
    lane = jnp.asarray(np.stack([i, j, r] + [0 * r] * 5), jnp.int32)
    short = np.arange(unit * most)
    every = np.arange(unit)
    gather = (short[None, :, None] == (i * most + r)[None, None, :]) & (j[None] == every[:, None])[:, None, :]
    gather, spread = jnp.asarray(gather, BF16), jnp.asarray(gather.transpose(0, 2, 1), BF16)

    block = (PIECES * most, width // PIECES)
    vmem = pl.BlockSpec(memory_space=pltpu.VMEM)
    hbm = pl.BlockSpec(memory_space=pl.ANY)
    dma = pltpu.SemaphoreType.DMA
    return pl.pallas_call(
        functools.partial(kernel, n, narrow, most, unit),
        out_shape=jax.ShapeDtypeStruct((tok_rows, width), BF16),
        in_specs=[vmem] * 4 + [hbm] * 8,
        out_specs=hbm,
        scratch_shapes=[
            pltpu.VMEM((tok_rows, width), BF16),
            pltpu.VMEM((rows, tok_rows), F32),
            pltpu.VMEM((rows, tok_rows), F32),
            pltpu.VMEM((unit, unit * most, rows), BF16),
            pltpu.VMEM((unit, rows, unit * most), BF16),
            pltpu.VMEM((width, hidden), BF16),
            pltpu.VMEM((width, hidden), BF16),
            pltpu.VMEM((hidden, width), BF16),
            pltpu.VMEM((tok_rows, width), BF16),
            pltpu.VMEM((3 * half,) + block, BF16),
            pltpu.VMEM((half + 2 * plane,) + block, BF16),
            pltpu.VMEM((half + 2 * plane,) + block, BF16),
            pltpu.VMEM((3 * half,) + block, BF16),
            pltpu.VMEM((2, tok_rows, width), BF16),
            pltpu.VMEM((2, tok_rows, width), BF16),
            pltpu.VMEM((tok_rows, width), BF16),
            pltpu.VMEM((half * most, width), BF16),
            pltpu.VMEM((half * most, hidden), BF16),
            pltpu.VMEM((half * most, hidden), BF16),
            pltpu.VMEM((tok_rows, unit * width // PIECES), F32),
            pltpu.VMEM((8, tok_rows), F32),
            pltpu.VMEM((3, 8, tok_rows), F32),
            pltpu.VMEM((1, lanes), F32),
            pltpu.VMEM((n, 1, lanes), F32),
            pltpu.VMEM((3, 8, lanes), F32),
            dma((3,)), dma((3, quads)), dma((3,)), dma((3, quads)), dma, dma((2, quads)), dma((2,)),
            dma((quads,)), dma, dma((2,)), dma, dma, dma((5,)), dma((3,)), dma((quads,)),
        ],
        compiler_params=pltpu.CompilerParams(
            collective_id=0, has_side_effects=True, vmem_limit_bytes=60 * 1024 * 1024
        ),
    )(expert_ids.T, gate_values.T, capacity[None], lane, tokens, code, turn, gather, spread, w_gate, w_up, w_down)


def solution(mesh):
    both = ("wide", "narrow")
    n, narrow = mesh.shape["wide"] * mesh.shape["narrow"], mesh.shape["narrow"]
    return jax.shard_map(
        functools.partial(on_device, n, narrow),
        mesh=mesh,
        in_specs=(P(both, None), P(both, None), P(both, None), P(),
                  P(both, None, None), P(both, None, None), P(both, None, None)),
        out_specs=P(both, None),
        check_vma=False,
    )
```

```python
import functools
import math

import jax
import jax.numpy as jnp
import numpy as np
from jax import lax
from jax.experimental import pallas as pl
from jax.experimental.pallas import tpu as pltpu
from jax.sharding import PartitionSpec as P

MESH = pl.DeviceIdType.MESH
PIECES = 16
PLANES = 4
F32 = jnp.float32
BF16 = jnp.bfloat16
NT = (((1,), (1,)), ((), ()))


def flip(me, off, bits):
    out = 0
    for b in range(bits):
        w = 1 << b
        out = out + (((me // w) % 2 + (off // w) % 2) % 2) * w
    return out


def kernel(n, narrow, most, unit, ids, gates, cap, lane, tok_hbm, code_hbm, turn_hbm, gather_hbm, spread_hbm,
           wg_hbm, wu_hbm, wd_hbm, out_hbm,
           tok, code, turn, gather, spread, wg, wu, wd, out,
           sent, came, back, home, hop, hop_back, far, mixed, stage, cross, x, h, h_own, total, note, meta, cnt, seen, left,
           s_sent, r_came, s_back, r_home, s_far, r_far, s_mixed, r_cross, s_stage, r_stage, s_hop, r_hop, s_note, r_note, s_cnt, r_cnt,
           lsem, wsem, osem):
    bits = int(math.log2(n))
    half, plane = n // 2, n // PLANES
    rows, part = unit * unit * most, unit * most
    tok_rows, width = tok.shape
    hidden = wg.shape[1]
    lanes = cnt.shape[1]
    piece = width // PIECES
    quads = PIECES // unit
    wide_cols = unit * piece
    me = lax.axis_index("wide") * narrow + lax.axis_index("narrow")
    place = me // plane
    inner = jnp.logical_or(place == 1, place == 2)
    is_inner = jnp.where(inner, 1, 0)
    relay_off = (2 + is_inner) * plane
    which = 1 - is_inner

    mine = [((me // (1 << b)) % 2) * (1 << b) for b in range(bits)]
    level = int(math.log2(plane))
    facing = list(mine)
    facing[level] = jnp.where(inner, mine[level], plane - mine[level])

    def where_is(off, origin=mine):
        if isinstance(off, int):
            peer = [(1 << b) - v if (off >> b) % 2 else v for b, v in enumerate(origin)]
            low = int(math.log2(narrow))
            return (sum(peer[low:]) // narrow, sum(peer[:low]))
        peer = flip(sum(origin), off, bits)
        return (peer // narrow, peer % narrow)

    def remote(src, dst, send, recv, off, origin=mine):
        return pltpu.make_async_remote_copy(
            src_ref=src, dst_ref=dst, send_sem=send, recv_sem=recv,
            device_id=where_is(off, origin), device_id_type=MESH)

    def each(first, last, body):
        if last - first <= 32:
            for off in range(first, last):
                body(off)
        else:
            pl.loop(first, last)(body)

    def groups(count, body):
        if unit <= 4:
            for g in range(count):
                body(g)
        else:
            pl.loop(0, count)(body)

    def columns(q, j):
        return pl.ds(pl.multiple_of((q * unit + j) * piece, piece), piece)

    def quad_columns(q):
        return pl.ds(pl.multiple_of(q * wide_cols, wide_cols), wide_cols)

    def quad_rows(q):
        return pl.ds(pl.multiple_of(q * part, part), part)

    barrier = pltpu.get_barrier_semaphore()

    with jax.named_scope("signals"):
        each(1, n, lambda off: pl.semaphore_signal(
            barrier, inc=1, device_id=where_is(off), device_id_type=MESH))

    inputs = [
        pltpu.make_async_copy(hbm, v, lsem.at[i])
        for i, (hbm, v) in enumerate(((tok_hbm, tok), (code_hbm, code), (turn_hbm, turn),
                                      (gather_hbm, gather), (spread_hbm, spread)))
    ]
    loads = [
        pltpu.make_async_copy(hbm.at[0], v, wsem.at[i])
        for i, (hbm, v) in enumerate(((wg_hbm, wg), (wu_hbm, wu), (wd_hbm, wd)))
    ]
    for load in inputs:
        load.start()

    names = [ids[c:c + 1, :] for c in (0, 1)]
    expert = lax.broadcasted_iota(jnp.int32, (lanes, tok_rows), 0)
    hot = [jnp.where(expert == name, 1.0, 0.0) for name in names]
    both = (hot[0] + hot[1]).astype(BF16)
    ahead = lax.broadcasted_iota(jnp.int32, (tok_rows, tok_rows), 0) < lax.broadcasted_iota(
        jnp.int32, (tok_rows, tok_rows), 1)
    before = jnp.dot(both, jnp.where(ahead, 1.0, 0.0).astype(BF16), preferred_element_type=F32)
    ranks = [jnp.sum(o * before, axis=0, keepdims=True) for o in hot]
    tally = lax.dot_general(jnp.ones((8, tok_rows), BF16), both, NT, preferred_element_type=F32)
    cnt[...] = tally[0:1, :]
    left[0] = jnp.zeros((8, lanes), F32)
    left[0, 0:1, 0:cap.shape[1]] = cap[...].astype(F32)
    limit = left[0, 0:1, :]
    seen[0] = tally[0:1, :]
    relay = flip(me, relay_off, bits)
    for host, ref in ((me, meta.at[0]), (relay, note)):
        slots = [((name ^ host) * most).astype(F32) + rank for name, rank in zip(names, ranks)]
        ref[0:1, :] = slots[0]
        ref[1:2, :] = slots[1]
        ref[2:4, :] = gates[...].astype(F32)

    for load in inputs:
        load.wait()

    with jax.named_scope("barrier"):
        pl.semaphore_wait(barrier, n - 1)

    for load in loads:
        load.start()

    note_copy = remote(note, meta.at[1 + which], s_note, r_note.at[which], relay_off)
    note_copy.start()

    each(1, n, lambda off: remote(cnt, seen.at[off], s_cnt, r_cnt, off).start())

    def far_copy(q):
        return remote(tok.at[:, quad_columns(q)], far.at[which, :, quad_columns(q)],
                      s_far, r_far.at[which, q], relay_off)

    def send_far():
        @pl.loop(0, quads)
        def _(q):
            far_copy(q).start()

    def aside(ref, hops, turn_back, q, off, send):
        if isinstance(off, int) and off == plane:
            hops[0, quad_rows(q), :] = ref[off, quad_rows(q), :]
        else:
            remote(ref.at[off, quad_rows(q), :], hops.at[off - plane, quad_rows(q), :],
                   send, r_hop.at[turn_back, q], off - plane).start()

    def pass_on(hops, into, turn_back, arrived):
        @pl.loop(0, quads)
        def _(q):
            with jax.named_scope(f"wait_hop{turn_back}"):
                block_copy(hops, 1, plane, q, s_hop.at[turn_back], r_hop.at[turn_back, q]).wait_recv()
            remote(hops.at[:, quad_rows(q), :], into.at[pl.ds(plane, plane), quad_rows(q), :],
                   s_hop.at[turn_back], arrived.at[0, q], plane).start()

    def pack(k, q, edge=False):
        slots = [meta[k, c:c + 1, :] for c in (0, 1)]
        base = 0 if k == 0 else half + (k - 1) * plane

        def group(g):
            acc = jnp.zeros((rows, piece), F32)
            for j in range(unit):
                mine = jnp.where(turn[...] == j, code[...] + jnp.asarray(g * part, F32), -1.0)
                hit = jnp.where(mine == slots[0], 1.0, 0.0) + jnp.where(mine == slots[1], 1.0, 0.0)
                put = hit.astype(BF16)
                values = tok[:, columns(q, j)] if k == 0 else far[k - 1, :, columns(q, j)]
                acc = acc + jnp.dot(put, values, preferred_element_type=F32)
            sent[pl.ds(k * half + g * unit, unit), quad_rows(q), :] = acc.astype(BF16).reshape(unit, part, piece)

        with jax.named_scope(f"pack{k}"):
            groups(half // unit, group)

        def deal(off):
            into = base + off if k == 0 else base + off % plane
            remote(sent.at[k * half + off, quad_rows(q), :], came.at[into, quad_rows(q), :],
                   s_sent.at[k], r_came.at[k, q], off).start()

        each(1, plane if edge else half, deal)
        if edge:
            aside(sent, hop, 0, q, plane, s_sent.at[0])
            each(plane + 1, half, lambda off: aside(sent, hop, 0, q, off, s_sent.at[0]))

        came[base, quad_rows(q), :] = sent[k * half, quad_rows(q), :]

    def pack_far(k, q):
        with jax.named_scope(f"wait_far{k}"):
            remote(tok.at[:, quad_columns(q)], far.at[k - 1, :, quad_columns(q)],
                   s_far, r_far.at[k - 1, q], relay_off).wait_recv()
        pack(k, q)

    def block_copy(ref, first, last, q, send, recv):
        piece_of = ref.at[pl.ds(first, last - first), quad_rows(q), :]
        return remote(piece_of, piece_of, send, recv, relay_off)

    def receive(k, first=0, last=quads):
        base = 0 if k == 0 else half + (k - 1) * plane
        blocks = half if k == 0 else plane

        @pl.loop(first, last)
        def _(q):
            with jax.named_scope(f"wait_came{k}"):
                if k == 0:
                    block_copy(came, 1, half, q, s_back.at[k], r_came.at[k, q]).wait_recv()
                else:
                    @pl.when(inner)
                    def _():
                        block_copy(came, base + 1, base + plane, q, s_back.at[k], r_came.at[k, q]).wait_recv()

                    @pl.when(jnp.logical_not(inner))
                    def _():
                        block_copy(came, base, base + plane, q, s_back.at[k], r_came.at[k, q]).wait_recv()

            def group(g):
                block = came[pl.ds(base + g * unit, unit), quad_rows(q), :].reshape(rows, piece)
                for j in range(unit):
                    x[pl.ds(g * part, part), columns(q, j)] = jnp.dot(
                        gather[j], block, preferred_element_type=F32).astype(BF16)

            with jax.named_scope(f"unpack{k}"):
                groups(blocks // unit, group)

    step = math.gcd(hidden, 256)
    tiles = hidden // step

    def gate_up(k, h, first=0, last=tiles):
        count = (half if k == 0 else plane) * most

        @pl.loop(first, last)
        def _(t):
            at = pl.ds(pl.multiple_of(t * step, step), step)
            with jax.named_scope(f"gate_up{k}"):
                gate = jnp.dot(x[0:count, :], wg[:, at], preferred_element_type=F32)
                up = jnp.dot(x[0:count, :], wu[:, at], preferred_element_type=F32)
                h[0:count, at] = (gate / (1.0 + jnp.exp(-gate)) * up).astype(BF16)

    def down_quad(k, h, q, edge=False):
        base = 0 if k == 0 else half + (k - 1) * plane
        blocks = half if k == 0 else plane
        count = blocks * most

        with jax.named_scope(f"down{k}"):
            for j in range(unit):
                x[0:count, j * piece:(j + 1) * piece] = jnp.dot(
                    h[0:count, :], wd[:, columns(q, j)], preferred_element_type=F32).astype(BF16)

        def group(g):
            acc = jnp.zeros((rows, piece), F32)
            for j in range(unit):
                acc = acc + jnp.dot(spread[j], x[pl.ds(g * part, part), j * piece:(j + 1) * piece],
                                    preferred_element_type=F32)
            back[pl.ds(base + g * unit, unit), quad_rows(q), :] = acc.astype(BF16).reshape(unit, part, piece)

        with jax.named_scope(f"spread{k}"):
            groups(blocks // unit, group)

        if k == 0:
            def answer(off):
                remote(back.at[off, quad_rows(q), :], home.at[off, quad_rows(q), :],
                       s_back.at[k], r_home.at[k, q], off).start()

            each(1, plane if edge else half, answer)
            if edge:
                aside(back, hop_back, 1, q, plane, s_back.at[0])
                each(plane + 1, half, lambda off: aside(back, hop_back, 1, q, off, s_back.at[0]))
            home[0, quad_rows(q), :] = back[0, quad_rows(q), :]
        else:
            def reply(low):
                off = low + (1 - is_inner) * plane
                remote(back.at[base + low, quad_rows(q), :], home.at[k * half + off, quad_rows(q), :],
                       s_back.at[k], r_home.at[k, q], low, facing).start()

            @pl.when(jnp.logical_not(inner))
            def _():
                reply(0)

            each(1, plane, reply)

            @pl.when(inner)
            def _():
                home[k * half, quad_rows(q), :] = back[base, quad_rows(q), :]

    def down(k, h, edge=False):
        @pl.loop(0, quads)
        def _(q):
            down_quad(k, h, q, edge)

    def rooms():
        remote(seen.at[pl.ds(1, n - 1)], seen.at[pl.ds(1, n - 1)], s_cnt, r_cnt, relay_off).wait_recv()
        sources = (me, flip(me, 3 * plane, bits), flip(me, 2 * plane, bits))

        def earlier(off, sums):
            peer = sum((1 << b) - v if (off >> b) % 2 else v for b, v in enumerate(mine)) if isinstance(
                off, int) else flip(me, off, bits)
            return tuple(t + seen[off] * jnp.where(peer < source, 1.0, 0.0) for t, source in zip(sums, sources))

        sums = tuple(jnp.zeros((1, lanes), F32) for _ in sources)
        if n <= 32:
            for off in range(n):
                sums = earlier(off, sums)
        else:
            sums = lax.fori_loop(0, n, earlier, sums)
        for k, taken in enumerate(sums):
            left[k] = jnp.broadcast_to(jnp.clip(limit - taken, 0.0, float(most)), (8, lanes))

    def combine(k, q):
        slots = [meta[k, c:c + 1, :] for c in (0, 1)]
        shares = [meta[k, c:c + 1, :] for c in (2, 3)]
        room_of = left[k].astype(BF16)
        eye = jnp.where(
            lax.broadcasted_iota(jnp.int32, (tok_rows, tok_rows), 0)
            == lax.broadcasted_iota(jnp.int32, (tok_rows, tok_rows), 1), 1.0, 0.0).astype(BF16)
        with jax.named_scope(f"wait_home{k}"):
            block_copy(home, k * half + 1, (k + 1) * half, q, s_back.at[k], r_home.at[k, q]).wait_recv()
        total[...] = jnp.zeros_like(total)

        def group(g):
            mine = code[...] + jnp.asarray(g * part, F32)
            weight = (jnp.where(mine == slots[0], shares[0], 0.0)
                      + jnp.where(mine == slots[1], shares[1], 0.0)).astype(BF16)
            weight = lax.dot_general(eye, weight, NT, preferred_element_type=F32)
            owner = lax.broadcasted_iota(jnp.int32, (lanes, rows), 0)
            pick = jnp.where(owner == ((lane[0:1, :] + g * unit) ^ me), 1.0, 0.0).astype(BF16)
            room = jnp.dot(room_of, pick, preferred_element_type=F32)[0:1, :]
            weight = jnp.where(room > lane[2:3, :].astype(F32), weight, 0.0)
            block = home[pl.ds(k * half + g * unit, unit), quad_rows(q), :].reshape(rows, piece)
            for j in range(unit):
                masked = jnp.where(lane[1:2, :] == j, weight, 0.0).astype(BF16)
                total[:, j * piece:(j + 1) * piece] += jnp.dot(masked, block, preferred_element_type=F32)

        with jax.named_scope(f"combine{k}"):
            groups(half // unit, group)

    def combine_far(k, q):
        combine(k, q)
        at = quad_columns(q)
        mixed[k - 1, :, at] = total[...].astype(BF16)
        into, arrived = (cross, r_cross) if k == 1 else (stage, r_stage)
        remote(mixed.at[k - 1, :, at], into.at[:, at], s_mixed.at[k - 1], arrived.at[q], 3 * plane).start()

    def forward(q):
        at = quad_columns(q)
        with jax.named_scope("wait_stage"):
            remote(stage.at[:, at], stage.at[:, at], s_stage, r_stage.at[q], relay_off).wait_recv()
        remote(stage.at[:, at], cross.at[:, at], s_stage, r_cross.at[q], plane).start()

    def pack_own(first, last, edge=False):
        @pl.loop(first, last)
        def _(q):
            pack(0, q, edge)

    def note_wait(k):
        with jax.named_scope("note"):
            remote(note, meta.at[k], s_note, r_note.at[k - 1], relay_off).wait_recv()

    def relay_in(k, first, last):
        @pl.loop(first, last)
        def _(q):
            pack_far(k, q)

    @pl.when(jnp.logical_not(inner))
    def _():
        send_far()

    @pl.when(jnp.logical_not(inner))
    def _():
        pack_own(0, quads, True)
        pass_on(hop, came, 0, r_came)

    @pl.when(inner)
    def _():
        pack_own(0, quads // 2)
        send_far()
        note_wait(2)

        @pl.loop(0, quads)
        def _(q):
            pack_far(2, q)

            @pl.when(q < quads - quads // 2)
            def _():
                pack(0, q + quads // 2)

    with jax.named_scope("rooms"):
        rooms()

    for load in loads:
        load.wait()

    early = max(1, quads // 4)
    late = max(early, quads - 1)

    @pl.when(inner)
    def _():
        note_wait(1)
        relay_in(1, 0, early)

    receive(2)
    gate_up(2, h)
    down(2, h)

    @pl.when(inner)
    def _():
        relay_in(1, early, late)

    receive(0)
    gate_up(0, h_own)

    def expert_one(first=0):
        receive(1, first)
        gate_up(1, h)
        down(1, h)

    def own_down(q):
        down_quad(0, h_own, q)

    @pl.when(inner)
    def _():
        relay_in(1, late, quads)
        second, first = functools.partial(combine_far, 2), functools.partial(combine_far, 1)
        if quads == 4:
            steps = [(second, 0), (own_down, 0), (own_down, 1), (second, 1), (receive, 1, 0, 2), (second, 2),
                     (second, 3), (forward, 0), (expert_one, 2), (forward, 1), (own_down, 2), (own_down, 3),
                     (forward, 2), (first, 0), (first, 1), (forward, 3), (first, 2), (first, 3)]
        else:
            steps = [(f, q) for f in (second, own_down) for q in range(quads)] + [(expert_one,)]
            steps += [(f, q) for f in (forward, first) for q in range(quads)]
        for act, *args in steps:
            act(*args)

    @pl.when(jnp.logical_not(inner))
    def _():
        expert_one()
        down(0, h_own, True)
        pass_on(hop_back, home, 1, r_home)

    @pl.loop(0, quads)
    def _(q):
        combine(0, q)
        at = quad_columns(q)
        with jax.named_scope("wait_cross"):
            remote(cross.at[:, at], cross.at[:, at], s_far, r_cross.at[q], relay_off).wait_recv()
        out[:, at] = (total[...] + cross[:, at].astype(F32)).astype(BF16)
        pltpu.make_async_copy(out.at[:, at], out_hbm.at[:, at], osem.at[q]).start()

    @pl.loop(0, quads)
    def _(q):
        at = quad_columns(q)
        pltpu.make_async_copy(out.at[:, at], out_hbm.at[:, at], osem.at[q]).wait()

    note_copy.wait_send()
    remote(seen.at[pl.ds(1, n - 1)], seen.at[pl.ds(1, n - 1)], s_cnt, r_cnt, relay_off).wait_send()
    remote(tok, cross, s_far, r_far.at[0, 0], relay_off).wait_send()

    def sent_all(ref, first, last, send):
        some = ref.at[pl.ds(first, last - first)]
        remote(some, some, send, r_cnt, relay_off).wait_send()

    @pl.when(inner)
    def _():
        sent_all(sent, 1, half, s_sent.at[0])
        sent_all(back, 1, half, s_back.at[0])
        for k in (1, 2):
            base = half + (k - 1) * plane
            sent_all(sent, k * half + 1, (k + 1) * half, s_sent.at[k])
            sent_all(back, base + 1, base + plane, s_back.at[k])
            remote(mixed.at[k - 1], cross, s_mixed.at[k - 1], r_cnt, relay_off).wait_send()
        remote(stage, cross, s_stage, r_cnt, relay_off).wait_send()

    @pl.when(jnp.logical_not(inner))
    def _():
        for ref, send in ((sent, s_sent.at[0]), (back, s_back.at[0])):
            sent_all(ref, 1, plane, send)
            sent_all(ref, plane + 1, half, send)
        sent_all(hop, 0, plane, s_hop.at[0])
        sent_all(hop_back, 0, plane, s_hop.at[1])
        for k in (1, 2):
            base = half + (k - 1) * plane
            sent_all(back, base, base + plane, s_back.at[k])


def on_device(n, narrow, tokens, expert_ids, gate_values, capacity, w_gate, w_up, w_down):
    experts = capacity.shape[0]
    tok_rows, width = tokens.shape
    hidden = w_gate.shape[2]
    most = 3 * tok_rows // experts
    unit = 16 // math.gcd(16, most)
    half, plane = n // 2, n // PLANES
    rows = unit * unit * most
    quads = PIECES // unit
    lanes = -(-experts // 128) * 128

    i, j, r = np.meshgrid(np.arange(unit), np.arange(unit), np.arange(most), indexing="ij")
    i, j, r = i.reshape(-1), j.reshape(-1), r.reshape(-1)
    code = jnp.asarray(np.broadcast_to((i * most + r)[:, None], (rows, tok_rows)), F32)
    turn = jnp.asarray(np.broadcast_to(j[:, None], (rows, tok_rows)), F32)
    lane = jnp.asarray(np.stack([i, j, r] + [0 * r] * 5), jnp.int32)
    short = np.arange(unit * most)
    every = np.arange(unit)
    gather = (short[None, :, None] == (i * most + r)[None, None, :]) & (j[None] == every[:, None])[:, None, :]
    gather, spread = jnp.asarray(gather, BF16), jnp.asarray(gather.transpose(0, 2, 1), BF16)

    block = (PIECES * most, width // PIECES)
    vmem = pl.BlockSpec(memory_space=pltpu.VMEM)
    hbm = pl.BlockSpec(memory_space=pl.ANY)
    dma = pltpu.SemaphoreType.DMA
    return pl.pallas_call(
        functools.partial(kernel, n, narrow, most, unit),
        out_shape=jax.ShapeDtypeStruct((tok_rows, width), BF16),
        in_specs=[vmem] * 4 + [hbm] * 8,
        out_specs=hbm,
        scratch_shapes=[
            pltpu.VMEM((tok_rows, width), BF16),
            pltpu.VMEM((rows, tok_rows), F32),
            pltpu.VMEM((rows, tok_rows), F32),
            pltpu.VMEM((unit, unit * most, rows), BF16),
            pltpu.VMEM((unit, rows, unit * most), BF16),
            pltpu.VMEM((width, hidden), BF16),
            pltpu.VMEM((width, hidden), BF16),
            pltpu.VMEM((hidden, width), BF16),
            pltpu.VMEM((tok_rows, width), BF16),
            pltpu.VMEM((3 * half,) + block, BF16),
            pltpu.VMEM((half + 2 * plane,) + block, BF16),
            pltpu.VMEM((half + 2 * plane,) + block, BF16),
            pltpu.VMEM((3 * half,) + block, BF16),
            pltpu.VMEM((plane,) + block, BF16),
            pltpu.VMEM((plane,) + block, BF16),
            pltpu.VMEM((2, tok_rows, width), BF16),
            pltpu.VMEM((2, tok_rows, width), BF16),
            pltpu.VMEM((tok_rows, width), BF16),
            pltpu.VMEM((tok_rows, width), BF16),
            pltpu.VMEM((half * most, width), BF16),
            pltpu.VMEM((half * most, hidden), BF16),
            pltpu.VMEM((half * most, hidden), BF16),
            pltpu.VMEM((tok_rows, unit * width // PIECES), F32),
            pltpu.VMEM((8, tok_rows), F32),
            pltpu.VMEM((3, 8, tok_rows), F32),
            pltpu.VMEM((1, lanes), F32),
            pltpu.VMEM((n, 1, lanes), F32),
            pltpu.VMEM((3, 8, lanes), F32),
            dma((3,)), dma((3, quads)), dma((3,)), dma((3, quads)), dma, dma((2, quads)), dma((2,)),
            dma((quads,)), dma, dma((quads,)), dma((2,)), dma((2, quads)), dma, dma((2,)), dma, dma, dma((5,)), dma((3,)), dma((quads,)),
        ],
        compiler_params=pltpu.CompilerParams(
            collective_id=0, has_side_effects=True, vmem_limit_bytes=60 * 1024 * 1024
        ),
    )(expert_ids.T, gate_values.T, capacity[None], lane, tokens, code, turn, gather, spread, w_gate, w_up, w_down)


def solution(mesh):
    both = ("wide", "narrow")
    n, narrow = mesh.shape["wide"] * mesh.shape["narrow"], mesh.shape["narrow"]
    return jax.shard_map(
        functools.partial(on_device, n, narrow),
        mesh=mesh,
        in_specs=(P(both, None), P(both, None), P(both, None), P(),
                  P(both, None, None), P(both, None, None), P(both, None, None)),
        out_specs=P(both, None),
        check_vma=False,
    )
```

```python
import functools
import math

import jax
import jax.numpy as jnp
import numpy as np
from jax import lax
from jax.experimental import pallas as pl
from jax.experimental.pallas import tpu as pltpu
from jax.sharding import PartitionSpec as P

MESH = pl.DeviceIdType.MESH
PIECES = 16
PLANES = 4
F32 = jnp.float32
BF16 = jnp.bfloat16
NT = (((1,), (1,)), ((), ()))


def flip(me, off, bits):
    out = 0
    for b in range(bits):
        w = 1 << b
        out = out + (((me // w) % 2 + (off // w) % 2) % 2) * w
    return out


def kernel(n, narrow, most, unit, ids_hbm, gates_hbm, cap_hbm, tok_hbm, lane_hbm, code_hbm, turn_hbm,
           gather_hbm, spread_hbm, wg_hbm, wu_hbm, wd_hbm, out,
           ids, gates, cap, tok, lane, code, turn, gather, spread, wg, wu, wd,
           sent, came, back, home, hop, hop_back, far, mixed, stage, cross, x, gates_up, h, h_own, total, note, meta, cnt, seen, left,
           s_sent, r_came, s_back, r_home, s_far, r_far, s_mixed, r_cross, s_stage, r_stage, s_hop, r_hop, s_note, r_note, s_cnt, r_cnt,
           lsem, wsem):
    bits = int(math.log2(n))
    half, plane = n // 2, n // PLANES
    rows, part = unit * unit * most, unit * most
    tok_rows, width = tok.shape
    hidden = wg.shape[1]
    lanes = cnt.shape[1]
    piece = width // PIECES
    quads = PIECES // unit
    wide_cols = unit * piece
    me = lax.axis_index("wide") * narrow + lax.axis_index("narrow")
    place = me // plane
    inner = jnp.logical_or(place == 1, place == 2)
    is_inner = jnp.where(inner, 1, 0)
    relay_off = (2 + is_inner) * plane
    which = 1 - is_inner

    mine = [((me // (1 << b)) % 2) * (1 << b) for b in range(bits)]
    level = int(math.log2(plane))
    facing = list(mine)
    facing[level] = jnp.where(inner, mine[level], plane - mine[level])

    def where_is(off, origin=mine):
        if isinstance(off, int):
            peer = [(1 << b) - v if (off >> b) % 2 else v for b, v in enumerate(origin)]
            low = int(math.log2(narrow))
            return (sum(peer[low:]) // narrow, sum(peer[:low]))
        peer = flip(sum(origin), off, bits)
        return (peer // narrow, peer % narrow)

    def remote(src, dst, send, recv, off, origin=mine):
        return pltpu.make_async_remote_copy(
            src_ref=src, dst_ref=dst, send_sem=send, recv_sem=recv,
            device_id=where_is(off, origin), device_id_type=MESH)

    def each(first, last, body):
        if last - first <= 32:
            for off in range(first, last):
                body(off)
        else:
            pl.loop(first, last)(body)

    def groups(count, body):
        if unit <= 4:
            for g in range(count):
                body(g)
        else:
            pl.loop(0, count)(body)

    def columns(q, j):
        return pl.ds(pl.multiple_of((q * unit + j) * piece, piece), piece)

    def quad_columns(q):
        return pl.ds(pl.multiple_of(q * wide_cols, wide_cols), wide_cols)

    def quad_rows(q):
        return pl.ds(pl.multiple_of(q * part, part), part)

    inputs = [
        pltpu.make_async_copy(hbm, v, lsem.at[i])
        for i, (hbm, v) in enumerate((
            (ids_hbm, ids), (gates_hbm, gates), (cap_hbm, cap), (tok_hbm, tok), (lane_hbm, lane),
            (code_hbm, code), (turn_hbm, turn), (gather_hbm, gather), (spread_hbm, spread)))
    ]
    for load in inputs:
        load.start()

    barrier = pltpu.get_barrier_semaphore()

    with jax.named_scope("signals"):
        each(1, n, lambda off: pl.semaphore_signal(
            barrier, inc=1, device_id=where_is(off), device_id_type=MESH))

    loads = [
        pltpu.make_async_copy(hbm.at[0], v, wsem.at[i])
        for i, (hbm, v) in enumerate(((wg_hbm, wg), (wu_hbm, wu), (wd_hbm, wd)))
    ]

    for load in inputs[:3]:
        load.wait()

    names = [ids[c:c + 1, :] for c in (0, 1)]
    expert = lax.broadcasted_iota(jnp.int32, (lanes, tok_rows), 0)
    hot = [jnp.where(expert == name, 1.0, 0.0) for name in names]
    both = (hot[0] + hot[1]).astype(BF16)
    ahead = lax.broadcasted_iota(jnp.int32, (tok_rows, tok_rows), 0) < lax.broadcasted_iota(
        jnp.int32, (tok_rows, tok_rows), 1)
    before = jnp.dot(both, jnp.where(ahead, 1.0, 0.0).astype(BF16), preferred_element_type=F32)
    ranks = [jnp.sum(o * before, axis=0, keepdims=True) for o in hot]
    tally = lax.dot_general(jnp.ones((8, tok_rows), BF16), both, NT, preferred_element_type=F32)
    cnt[...] = tally[0:1, :]
    left[0] = jnp.zeros((8, lanes), F32)
    left[0, 0:1, 0:cap.shape[1]] = cap[...].astype(F32)
    limit = left[0, 0:1, :]
    seen[0] = tally[0:1, :]
    relay = flip(me, relay_off, bits)
    for host, ref in ((me, meta.at[0]), (relay, note)):
        slots = [((name ^ host) * most).astype(F32) + rank for name, rank in zip(names, ranks)]
        ref[0:1, :] = slots[0]
        ref[1:2, :] = slots[1]
        ref[2:4, :] = gates[...].astype(F32)

    for load in inputs[3:]:
        load.wait()

    with jax.named_scope("barrier"):
        pl.semaphore_wait(barrier, n - 1)

    for load in loads:
        load.start()

    note_copy = remote(note, meta.at[1 + which], s_note, r_note.at[which], relay_off)
    note_copy.start()

    each(1, n, lambda off: remote(cnt, seen.at[off], s_cnt, r_cnt, off).start())

    def far_copy(q):
        return remote(tok.at[:, quad_columns(q)], far.at[which, :, quad_columns(q)],
                      s_far, r_far.at[which, q], relay_off)

    def send_far():
        @pl.loop(0, quads)
        def _(q):
            far_copy(q).start()

    def aside(ref, hops, turn_back, q, off, send):
        if isinstance(off, int) and off == plane:
            hops[0, quad_rows(q), :] = ref[off, quad_rows(q), :]
        else:
            remote(ref.at[off, quad_rows(q), :], hops.at[off - plane, quad_rows(q), :],
                   send, r_hop.at[turn_back, q], off - plane).start()

    def pass_on(hops, into, turn_back, arrived, q):
        with jax.named_scope(f"wait_hop{turn_back}"):
            block_copy(hops, 1, plane, q, s_hop.at[turn_back], r_hop.at[turn_back, q]).wait_recv()
        remote(hops.at[:, quad_rows(q), :], into.at[pl.ds(plane, plane), quad_rows(q), :],
               s_hop.at[turn_back], arrived.at[0, q], plane).start()

    def pack(k, q, edge=False):
        slots = [meta[k, c:c + 1, :] for c in (0, 1)]
        base = 0 if k == 0 else half + (k - 1) * plane

        def group(g):
            acc = jnp.zeros((rows, piece), F32)
            for j in range(unit):
                mine = jnp.where(turn[...] == j, code[...] + jnp.asarray(g * part, F32), -1.0)
                hit = jnp.where(mine == slots[0], 1.0, 0.0) + jnp.where(mine == slots[1], 1.0, 0.0)
                put = hit.astype(BF16)
                values = tok[:, columns(q, j)] if k == 0 else far[k - 1, :, columns(q, j)]
                acc = acc + jnp.dot(put, values, preferred_element_type=F32)
            sent[pl.ds(k * half + g * unit, unit), quad_rows(q), :] = acc.astype(BF16).reshape(unit, part, piece)

        with jax.named_scope(f"pack{k}"):
            groups(half // unit, group)

        def deal(off):
            into = base + off if k == 0 else base + off % plane
            remote(sent.at[k * half + off, quad_rows(q), :], came.at[into, quad_rows(q), :],
                   s_sent.at[k], r_came.at[k, q], off).start()

        each(1, plane if edge else half, deal)
        if edge:
            aside(sent, hop, 0, q, plane, s_sent.at[0])
            each(plane + 1, half, lambda off: aside(sent, hop, 0, q, off, s_sent.at[0]))

        came[base, quad_rows(q), :] = sent[k * half, quad_rows(q), :]

    def pack_far(k, q):
        with jax.named_scope(f"wait_far{k}"):
            remote(tok.at[:, quad_columns(q)], far.at[k - 1, :, quad_columns(q)],
                   s_far, r_far.at[k - 1, q], relay_off).wait_recv()
        pack(k, q)

    def block_copy(ref, first, last, q, send, recv):
        piece_of = ref.at[pl.ds(first, last - first), quad_rows(q), :]
        return remote(piece_of, piece_of, send, recv, relay_off)

    step = math.gcd(hidden, 256)
    tiles = hidden // step

    def tile(t):
        return pl.ds(pl.multiple_of(t * step, step), step)

    def receive(k, first=0, last=quads, after=None, partial=False):
        base = 0 if k == 0 else half + (k - 1) * plane
        blocks = half if k == 0 else plane
        count = blocks * most
        if partial and first == 0:
            gates_up[:, 0:count, :] = jnp.zeros((2, count, hidden), F32)

        @pl.loop(first, last)
        def _(q):
            with jax.named_scope(f"wait_came{k}"):
                if k == 0:
                    block_copy(came, 1, half, q, s_back.at[k], r_came.at[k, q]).wait_recv()
                else:
                    @pl.when(inner)
                    def _():
                        block_copy(came, base + 1, base + plane, q, s_back.at[k], r_came.at[k, q]).wait_recv()

                    @pl.when(jnp.logical_not(inner))
                    def _():
                        block_copy(came, base, base + plane, q, s_back.at[k], r_came.at[k, q]).wait_recv()

            if after is not None:
                after(q)

            def group(g):
                block = came[pl.ds(base + g * unit, unit), quad_rows(q), :].reshape(rows, piece)
                for j in range(unit):
                    at = slice(j * piece, (j + 1) * piece) if partial else columns(q, j)
                    x[pl.ds(g * part, part), at] = jnp.dot(
                        gather[j], block, preferred_element_type=F32).astype(BF16)

            with jax.named_scope(f"unpack{k}"):
                groups(blocks // unit, group)

            if partial:
                with jax.named_scope(f"gate_up{k}"):
                    for t in range(tiles):
                        for i, w in enumerate((wg, wu)):
                            gates_up[i, 0:count, t * step:(t + 1) * step] += jnp.dot(
                                x[0:count, 0:wide_cols], w[quad_columns(q), t * step:(t + 1) * step],
                                preferred_element_type=F32)

    def activate(k, h, partial=False):
        count = (half if k == 0 else plane) * most

        @pl.loop(0, tiles)
        def _(t):
            with jax.named_scope(f"activate{k}"):
                if partial:
                    gate, up = gates_up[0, 0:count, tile(t)], gates_up[1, 0:count, tile(t)]
                else:
                    gate = jnp.dot(x[0:count, :], wg[:, tile(t)], preferred_element_type=F32)
                    up = jnp.dot(x[0:count, :], wu[:, tile(t)], preferred_element_type=F32)
                h[0:count, tile(t)] = (gate / (1.0 + jnp.exp(-gate)) * up).astype(BF16)

    def down_quad(k, h, q, edge=False):
        base = 0 if k == 0 else half + (k - 1) * plane
        blocks = half if k == 0 else plane
        count = blocks * most

        with jax.named_scope(f"down{k}"):
            for j in range(unit):
                x[0:count, j * piece:(j + 1) * piece] = jnp.dot(
                    h[0:count, :], wd[:, columns(q, j)], preferred_element_type=F32).astype(BF16)

        def group(g):
            acc = jnp.zeros((rows, piece), F32)
            for j in range(unit):
                acc = acc + jnp.dot(spread[j], x[pl.ds(g * part, part), j * piece:(j + 1) * piece],
                                    preferred_element_type=F32)
            back[pl.ds(base + g * unit, unit), quad_rows(q), :] = acc.astype(BF16).reshape(unit, part, piece)

        with jax.named_scope(f"spread{k}"):
            groups(blocks // unit, group)

        if k == 0:
            def answer(off):
                remote(back.at[off, quad_rows(q), :], home.at[off, quad_rows(q), :],
                       s_back.at[k], r_home.at[k, q], off).start()

            each(1, plane if edge else half, answer)
            if edge:
                aside(back, hop_back, 1, q, plane, s_back.at[0])
                each(plane + 1, half, lambda off: aside(back, hop_back, 1, q, off, s_back.at[0]))
            home[0, quad_rows(q), :] = back[0, quad_rows(q), :]
        else:
            def reply(low):
                off = low + (1 - is_inner) * plane
                remote(back.at[base + low, quad_rows(q), :], home.at[k * half + off, quad_rows(q), :],
                       s_back.at[k], r_home.at[k, q], low, facing).start()

            @pl.when(jnp.logical_not(inner))
            def _():
                reply(0)

            each(1, plane, reply)

            @pl.when(inner)
            def _():
                home[k * half, quad_rows(q), :] = back[base, quad_rows(q), :]

    def down(k, h, edge=False):
        @pl.loop(0, quads)
        def _(q):
            down_quad(k, h, q, edge)

    def rooms():
        remote(seen.at[pl.ds(1, n - 1)], seen.at[pl.ds(1, n - 1)], s_cnt, r_cnt, relay_off).wait_recv()
        sources = (me, flip(me, 3 * plane, bits), flip(me, 2 * plane, bits))

        def earlier(off, sums):
            peer = sum((1 << b) - v if (off >> b) % 2 else v for b, v in enumerate(mine)) if isinstance(
                off, int) else flip(me, off, bits)
            return tuple(t + seen[off] * jnp.where(peer < source, 1.0, 0.0) for t, source in zip(sums, sources))

        sums = tuple(jnp.zeros((1, lanes), F32) for _ in sources)
        if n <= 32:
            for off in range(n):
                sums = earlier(off, sums)
        else:
            sums = lax.fori_loop(0, n, earlier, sums)
        for k, taken in enumerate(sums):
            left[k] = jnp.broadcast_to(jnp.clip(limit - taken, 0.0, float(most)), (8, lanes))

    def combine(k, q):
        slots = [meta[k, c:c + 1, :] for c in (0, 1)]
        shares = [meta[k, c:c + 1, :] for c in (2, 3)]
        room_of = left[k].astype(BF16)
        eye = jnp.where(
            lax.broadcasted_iota(jnp.int32, (tok_rows, tok_rows), 0)
            == lax.broadcasted_iota(jnp.int32, (tok_rows, tok_rows), 1), 1.0, 0.0).astype(BF16)
        with jax.named_scope(f"wait_home{k}"):
            block_copy(home, k * half + 1, (k + 1) * half, q, s_back.at[k], r_home.at[k, q]).wait_recv()
        total[...] = jnp.zeros_like(total)

        def group(g):
            mine = code[...] + jnp.asarray(g * part, F32)
            weight = (jnp.where(mine == slots[0], shares[0], 0.0)
                      + jnp.where(mine == slots[1], shares[1], 0.0)).astype(BF16)
            weight = lax.dot_general(eye, weight, NT, preferred_element_type=F32)
            owner = lax.broadcasted_iota(jnp.int32, (lanes, rows), 0)
            pick = jnp.where(owner == ((lane[0:1, :] + g * unit) ^ me), 1.0, 0.0).astype(BF16)
            room = jnp.dot(room_of, pick, preferred_element_type=F32)[0:1, :]
            weight = jnp.where(room > lane[2:3, :].astype(F32), weight, 0.0)
            block = home[pl.ds(k * half + g * unit, unit), quad_rows(q), :].reshape(rows, piece)
            for j in range(unit):
                masked = jnp.where(lane[1:2, :] == j, weight, 0.0).astype(BF16)
                total[:, j * piece:(j + 1) * piece] += jnp.dot(masked, block, preferred_element_type=F32)

        with jax.named_scope(f"combine{k}"):
            groups(half // unit, group)

    def combine_far(k, q):
        combine(k, q)
        at = quad_columns(q)
        mixed[k - 1, :, at] = total[...].astype(BF16)
        into, arrived = (cross, r_cross) if k == 1 else (stage, r_stage)
        remote(mixed.at[k - 1, :, at], into.at[:, at], s_mixed.at[k - 1], arrived.at[q], 3 * plane).start()

    def forward(q):
        at = quad_columns(q)
        with jax.named_scope("wait_stage"):
            remote(stage.at[:, at], stage.at[:, at], s_stage, r_stage.at[q], relay_off).wait_recv()
        remote(stage.at[:, at], cross.at[:, at], s_stage, r_cross.at[q], plane).start()

    def pack_own(first, last, edge=False):
        @pl.loop(first, last)
        def _(q):
            pack(0, q, edge)

    def note_wait(k):
        with jax.named_scope("note"):
            remote(note, meta.at[k], s_note, r_note.at[k - 1], relay_off).wait_recv()

    def relay_in(k, first, last):
        @pl.loop(first, last)
        def _(q):
            pack_far(k, q)

    @pl.when(jnp.logical_not(inner))
    def _():
        send_far()

    early = max(1, quads // 4)
    late = max(early, quads - 1)

    def loaded():
        for load in loads:
            load.wait()

    @pl.when(jnp.logical_not(inner))
    def _():
        pack_own(0, quads, True)
        loaded()

        receive(2, after=lambda q: pass_on(hop, came, 0, r_came, q), partial=True)
        activate(2, h, True)
        down(2, h)
        with jax.named_scope("rooms"):
            rooms()

    @pl.when(inner)
    def _():
        pack_own(0, quads // 2)
        send_far()
        note_wait(2)
        relay_in(2, 0, quads)
        pack_own(quads // 2, quads)
        with jax.named_scope("rooms"):
            rooms()
        loaded()
        note_wait(1)
        relay_in(1, 0, early)
        receive(2)
        activate(2, h)
        down(2, h)
        relay_in(1, early, late)

    receive(0)
    activate(0, h_own)

    def receive_one(first, last, after=None):
        receive(1, first, last, after, partial=True)

    def expert_one(first=0, after=None):
        receive_one(first, quads, after)
        activate(1, h, True)
        down(1, h)

    def own_down(q):
        down_quad(0, h_own, q)

    @pl.when(inner)
    def _():
        relay_in(1, late, quads)
        second, first = functools.partial(combine_far, 2), functools.partial(combine_far, 1)
        if quads == 4:
            steps = [(second, 0), (own_down, 0), (own_down, 1), (second, 1), (receive_one, 0, 2), (second, 2),
                     (second, 3), (forward, 0), (expert_one, 2), (forward, 1), (own_down, 2), (own_down, 3),
                     (forward, 2), (first, 0), (first, 1), (forward, 3), (first, 2), (first, 3)]
        else:
            steps = [(f, q) for f in (second, own_down) for q in range(quads)] + [(expert_one,)]
            steps += [(f, q) for f in (forward, first) for q in range(quads)]
        for act, *args in steps:
            act(*args)

    @pl.when(jnp.logical_not(inner))
    def _():
        down(0, h_own, True)

        def hop_back_on(q):
            pass_on(hop_back, home, 1, r_home, q)

        def first_back(q):
            @pl.when(q == quads - 2)
            def _():
                hop_back_on(0)

        expert_one(after=first_back)
        pl.loop(min(1, quads - 1), quads)(hop_back_on)

    @pl.loop(0, quads)
    def _(q):
        combine(0, q)
        at = quad_columns(q)
        with jax.named_scope("wait_cross"):
            remote(cross.at[:, at], cross.at[:, at], s_far, r_cross.at[q], relay_off).wait_recv()
        out[:, at] = (total[...] + cross[:, at].astype(F32)).astype(BF16)

    note_copy.wait_send()
    remote(seen.at[pl.ds(1, n - 1)], seen.at[pl.ds(1, n - 1)], s_cnt, r_cnt, relay_off).wait_send()
    remote(tok, cross, s_far, r_far.at[0, 0], relay_off).wait_send()

    def sent_all(ref, first, last, send):
        some = ref.at[pl.ds(first, last - first)]
        remote(some, some, send, r_cnt, relay_off).wait_send()

    @pl.when(inner)
    def _():
        sent_all(sent, 1, half, s_sent.at[0])
        sent_all(back, 1, half, s_back.at[0])
        for k in (1, 2):
            base = half + (k - 1) * plane
            sent_all(sent, k * half + 1, (k + 1) * half, s_sent.at[k])
            sent_all(back, base + 1, base + plane, s_back.at[k])
            remote(mixed.at[k - 1], cross, s_mixed.at[k - 1], r_cnt, relay_off).wait_send()
        remote(stage, cross, s_stage, r_cnt, relay_off).wait_send()

    @pl.when(jnp.logical_not(inner))
    def _():
        for ref, send in ((sent, s_sent.at[0]), (back, s_back.at[0])):
            sent_all(ref, 1, plane, send)
            sent_all(ref, plane + 1, half, send)
        sent_all(hop, 0, plane, s_hop.at[0])
        sent_all(hop_back, 0, plane, s_hop.at[1])
        for k in (1, 2):
            base = half + (k - 1) * plane
            sent_all(back, base, base + plane, s_back.at[k])


def on_device(n, narrow, tokens, expert_ids, gate_values, capacity, w_gate, w_up, w_down):
    experts = capacity.shape[0]
    tok_rows, width = tokens.shape
    hidden = w_gate.shape[2]
    most = 3 * tok_rows // experts
    unit = 16 // math.gcd(16, most)
    half, plane = n // 2, n // PLANES
    rows = unit * unit * most
    quads = PIECES // unit
    lanes = -(-experts // 128) * 128

    i, j, r = np.meshgrid(np.arange(unit), np.arange(unit), np.arange(most), indexing="ij")
    i, j, r = i.reshape(-1), j.reshape(-1), r.reshape(-1)
    code = jnp.asarray(np.broadcast_to((i * most + r)[:, None], (rows, tok_rows)), F32)
    turn = jnp.asarray(np.broadcast_to(j[:, None], (rows, tok_rows)), F32)
    lane = jnp.asarray(np.stack([i, j, r] + [0 * r] * 5), jnp.int32)
    short = np.arange(unit * most)
    every = np.arange(unit)
    gather = (short[None, :, None] == (i * most + r)[None, None, :]) & (j[None] == every[:, None])[:, None, :]
    gather, spread = jnp.asarray(gather, BF16), jnp.asarray(gather.transpose(0, 2, 1), BF16)

    operands = [
        pltpu.with_memory_space_constraint(a, pltpu.HBM)
        for a in (expert_ids.T, gate_values.T, capacity[None], tokens, lane, code, turn, gather, spread,
                  w_gate, w_up, w_down)
    ]
    block = (PIECES * most, width // PIECES)
    vmem = pl.BlockSpec(memory_space=pltpu.VMEM)
    hbm = pl.BlockSpec(memory_space=pltpu.HBM)
    dma = pltpu.SemaphoreType.DMA
    return pl.pallas_call(
        functools.partial(kernel, n, narrow, most, unit),
        out_shape=jax.ShapeDtypeStruct((tok_rows, width), BF16),
        in_specs=[hbm] * 12,
        out_specs=vmem,
        scratch_shapes=[
            pltpu.VMEM((2, tok_rows), jnp.int32),
            pltpu.VMEM((2, tok_rows), BF16),
            pltpu.VMEM((1, experts), jnp.int32),
            pltpu.VMEM((tok_rows, width), BF16),
            pltpu.VMEM((8, rows), jnp.int32),
            pltpu.VMEM((rows, tok_rows), F32),
            pltpu.VMEM((rows, tok_rows), F32),
            pltpu.VMEM((unit, unit * most, rows), BF16),
            pltpu.VMEM((unit, rows, unit * most), BF16),
            pltpu.VMEM((width, hidden), BF16),
            pltpu.VMEM((width, hidden), BF16),
            pltpu.VMEM((hidden, width), BF16),
            pltpu.VMEM((3 * half,) + block, BF16),
            pltpu.VMEM((half + 2 * plane,) + block, BF16),
            pltpu.VMEM((half + 2 * plane,) + block, BF16),
            pltpu.VMEM((3 * half,) + block, BF16),
            pltpu.VMEM((plane,) + block, BF16),
            pltpu.VMEM((plane,) + block, BF16),
            pltpu.VMEM((2, tok_rows, width), BF16),
            pltpu.VMEM((2, tok_rows, width), BF16),
            pltpu.VMEM((tok_rows, width), BF16),
            pltpu.VMEM((tok_rows, width), BF16),
            pltpu.VMEM((half * most, width), BF16),
            pltpu.VMEM((2, half * most, hidden), F32),
            pltpu.VMEM((half * most, hidden), BF16),
            pltpu.VMEM((half * most, hidden), BF16),
            pltpu.VMEM((tok_rows, unit * width // PIECES), F32),
            pltpu.VMEM((8, tok_rows), F32),
            pltpu.VMEM((3, 8, tok_rows), F32),
            pltpu.VMEM((1, lanes), F32),
            pltpu.VMEM((n, 1, lanes), F32),
            pltpu.VMEM((3, 8, lanes), F32),
            dma((3,)), dma((3, quads)), dma((3,)), dma((3, quads)), dma, dma((2, quads)), dma((2,)),
            dma((quads,)), dma, dma((quads,)), dma((2,)), dma((2, quads)), dma, dma((2,)), dma, dma, dma((9,)), dma((3,)),
        ],
        compiler_params=pltpu.CompilerParams(
            collective_id=0, has_side_effects=True, vmem_limit_bytes=(52 if quads > 1 else 60) * 1024 * 1024
        ),
    )(*operands)


def solution(mesh):
    both = ("wide", "narrow")
    n, narrow = mesh.shape["wide"] * mesh.shape["narrow"], mesh.shape["narrow"]
    return jax.shard_map(
        functools.partial(on_device, n, narrow),
        mesh=mesh,
        in_specs=(P(both, None), P(both, None), P(both, None), P(),
                  P(both, None, None), P(both, None, None), P(both, None, None)),
        out_specs=P(both, None),
        check_vma=False,
    )
```

```python
import functools
import math

import jax
import jax.numpy as jnp
import numpy as np
from jax import lax
from jax.experimental import pallas as pl
from jax.experimental.pallas import tpu as pltpu
from jax.sharding import PartitionSpec as P

MESH = pl.DeviceIdType.MESH
PIECES = 16
PLANES = 4
F32 = jnp.float32
BF16 = jnp.bfloat16
NT = (((1,), (1,)), ((), ()))


def flip(me, off, bits):
    out = 0
    for b in range(bits):
        w = 1 << b
        out = out + (((me // w) % 2 + (off // w) % 2) % 2) * w
    return out


def kernel(n, narrow, most, unit, ids_hbm, gates_hbm, cap_hbm, tok_hbm, lane_hbm, code_hbm, turn_hbm,
           gather_hbm, spread_hbm, wg_hbm, wu_hbm, wd_hbm, out,
           ids, gates, cap, tok, lane, code, turn, gather, spread, wg, wu, wd,
           sent, came, back, home, hop, hop_back, far, mixed, stage, cross, x, gates_up, h, h_own, total, note, meta, cnt, seen, left,
           s_sent, r_came, s_back, r_home, s_far, r_far, s_mixed, r_cross, s_stage, r_stage, s_hop, r_hop, s_note, r_note, s_cnt, r_cnt, s_pass, r_source,
           lsem, wsem):
    bits = int(math.log2(n))
    half, plane = n // 2, n // PLANES
    rows, part = unit * unit * most, unit * most
    tok_rows, width = tok.shape
    hidden = wg.shape[1]
    lanes = cnt.shape[1]
    piece = width // PIECES
    quads = PIECES // unit
    wide_cols = unit * piece
    me = lax.axis_index("wide") * narrow + lax.axis_index("narrow")
    place = me // plane
    inner = jnp.logical_or(place == 1, place == 2)
    is_inner = jnp.where(inner, 1, 0)
    relay_off = (2 + is_inner) * plane
    which = 1 - is_inner

    mine = [((me // (1 << b)) % 2) * (1 << b) for b in range(bits)]
    level = int(math.log2(plane))
    facing = list(mine)
    facing[level] = jnp.where(inner, mine[level], plane - mine[level])

    def where_is(off, origin=mine):
        if isinstance(off, int):
            peer = [(1 << b) - v if (off >> b) % 2 else v for b, v in enumerate(origin)]
            low = int(math.log2(narrow))
            return (sum(peer[low:]) // narrow, sum(peer[:low]))
        peer = flip(sum(origin), off, bits)
        return (peer // narrow, peer % narrow)

    def remote(src, dst, send, recv, off, origin=mine):
        return pltpu.make_async_remote_copy(
            src_ref=src, dst_ref=dst, send_sem=send, recv_sem=recv,
            device_id=where_is(off, origin), device_id_type=MESH)

    def each(first, last, body):
        if last - first <= 32:
            for off in range(first, last):
                body(off)
        else:
            pl.loop(first, last)(body)

    def groups(count, body):
        if unit <= 4:
            for g in range(count):
                body(g)
        else:
            pl.loop(0, count)(body)

    def columns(q, j):
        return pl.ds(pl.multiple_of((q * unit + j) * piece, piece), piece)

    def quad_columns(q):
        return pl.ds(pl.multiple_of(q * wide_cols, wide_cols), wide_cols)

    def quad_rows(q):
        return pl.ds(pl.multiple_of(q * part, part), part)

    inputs = [
        pltpu.make_async_copy(hbm, v, lsem.at[i])
        for i, (hbm, v) in enumerate((
            (ids_hbm, ids), (gates_hbm, gates), (cap_hbm, cap), (tok_hbm, tok), (lane_hbm, lane),
            (code_hbm, code), (turn_hbm, turn), (gather_hbm, gather), (spread_hbm, spread)))
    ]
    for load in inputs:
        load.start()

    barrier = pltpu.get_barrier_semaphore()

    with jax.named_scope("signals"):
        def greet(off):
            pl.semaphore_signal(barrier, inc=1, device_id=where_is(off), device_id_type=MESH)

        each(1, half, greet)
        greet(2 * plane)

        @pl.when(inner)
        def _():
            greet(3 * plane)

    loads = [
        pltpu.make_async_copy(hbm.at[0], v, wsem.at[i])
        for i, (hbm, v) in enumerate(((wg_hbm, wg), (wu_hbm, wu), (wd_hbm, wd)))
    ]

    for load in inputs[:3]:
        load.wait()

    names = [ids[c:c + 1, :] for c in (0, 1)]
    expert = lax.broadcasted_iota(jnp.int32, (lanes, tok_rows), 0)
    hot = [jnp.where(expert == name, 1.0, 0.0) for name in names]
    both = (hot[0] + hot[1]).astype(BF16)
    ahead = lax.broadcasted_iota(jnp.int32, (tok_rows, tok_rows), 0) < lax.broadcasted_iota(
        jnp.int32, (tok_rows, tok_rows), 1)
    before = jnp.dot(both, jnp.where(ahead, 1.0, 0.0).astype(BF16), preferred_element_type=F32)
    ranks = [jnp.sum(o * before, axis=0, keepdims=True) for o in hot]
    tally = lax.dot_general(jnp.ones((8, tok_rows), BF16), both, NT, preferred_element_type=F32)
    cnt[...] = tally[0:1, :]
    left[0] = jnp.zeros((8, lanes), F32)
    left[0, 0:1, 0:cap.shape[1]] = cap[...].astype(F32)
    limit = left[0, 0:1, :]
    seen[0] = tally[0:1, :]
    relay = flip(me, relay_off, bits)
    for host, ref in ((me, meta.at[0]), (relay, note)):
        slots = [((name ^ host) * most).astype(F32) + rank for name, rank in zip(names, ranks)]
        ref[0:1, :] = slots[0]
        ref[1:2, :] = slots[1]
        ref[2:4, :] = gates[...].astype(F32)

    for load in inputs[3:]:
        load.wait()

    with jax.named_scope("barrier"):
        pl.semaphore_wait(barrier, half + is_inner)

    for load in loads:
        load.start()

    note_copy = remote(note, meta.at[1 + which], s_note, r_note.at[which], relay_off)
    note_copy.start()

    remote(cnt, seen.at[relay_off], s_cnt, r_source.at[which], relay_off).start()
    each(1, half, lambda off: remote(cnt, seen.at[off], s_cnt, r_cnt, off).start())

    def pass_counts(k):
        source = (4 - k) * plane
        remote(seen.at[source], seen.at[source], s_pass, r_source.at[k - 1], relay_off).wait_recv()

        def tell(off):
            into = source ^ off if isinstance(off, int) else flip(source, off, bits)
            remote(seen.at[source], seen.at[into], s_pass, r_cnt, off).start()

        each(1, half, tell)

    def counted(entries, send, recv):
        some = seen.at[pl.ds(0, entries)]
        return remote(some, some, send, recv, relay_off)

    def far_copy(q):
        return remote(tok.at[:, quad_columns(q)], far.at[which, :, quad_columns(q)],
                      s_far, r_far.at[which, q], relay_off)

    def send_far():
        @pl.loop(0, quads)
        def _(q):
            far_copy(q).start()

    def aside(ref, hops, turn_back, q, off, send):
        if isinstance(off, int) and off == plane:
            hops[0, quad_rows(q), :] = ref[off, quad_rows(q), :]
        else:
            remote(ref.at[off, quad_rows(q), :], hops.at[off - plane, quad_rows(q), :],
                   send, r_hop.at[turn_back, q], off - plane).start()

    def pass_on(hops, into, turn_back, arrived, q):
        with jax.named_scope(f"wait_hop{turn_back}"):
            block_copy(hops, 1, plane, q, s_hop.at[turn_back], r_hop.at[turn_back, q]).wait_recv()
        remote(hops.at[:, quad_rows(q), :], into.at[pl.ds(plane, plane), quad_rows(q), :],
               s_hop.at[turn_back], arrived.at[0, q], plane).start()

    def pack(k, q, edge=False):
        slots = [meta[k, c:c + 1, :] for c in (0, 1)]
        base = 0 if k == 0 else half + (k - 1) * plane

        def group(g):
            acc = jnp.zeros((rows, piece), F32)
            for j in range(unit):
                mine = jnp.where(turn[...] == j, code[...] + jnp.asarray(g * part, F32), -1.0)
                hit = jnp.where(mine == slots[0], 1.0, 0.0) + jnp.where(mine == slots[1], 1.0, 0.0)
                put = hit.astype(BF16)
                values = tok[:, columns(q, j)] if k == 0 else far[k - 1, :, columns(q, j)]
                acc = acc + jnp.dot(put, values, preferred_element_type=F32)
            sent[pl.ds(k * half + g * unit, unit), quad_rows(q), :] = acc.astype(BF16).reshape(unit, part, piece)

        with jax.named_scope(f"pack{k}"):
            groups(half // unit, group)

        def deal(off):
            into = base + off if k == 0 else base + off % plane
            remote(sent.at[k * half + off, quad_rows(q), :], came.at[into, quad_rows(q), :],
                   s_sent.at[k], r_came.at[k, q], off).start()

        each(1, plane if edge else half, deal)
        if edge:
            aside(sent, hop, 0, q, plane, s_sent.at[0])
            each(plane + 1, half, lambda off: aside(sent, hop, 0, q, off, s_sent.at[0]))

        came[base, quad_rows(q), :] = sent[k * half, quad_rows(q), :]

    def pack_far(k, q):
        with jax.named_scope(f"wait_far{k}"):
            remote(tok.at[:, quad_columns(q)], far.at[k - 1, :, quad_columns(q)],
                   s_far, r_far.at[k - 1, q], relay_off).wait_recv()
        pack(k, q)

    def block_copy(ref, first, last, q, send, recv):
        piece_of = ref.at[pl.ds(first, last - first), quad_rows(q), :]
        return remote(piece_of, piece_of, send, recv, relay_off)

    step = math.gcd(hidden, 256)
    tiles = hidden // step

    def tile(t):
        return pl.ds(pl.multiple_of(t * step, step), step)

    def receive(k, first=0, last=quads, after=None, partial=False):
        base = 0 if k == 0 else half + (k - 1) * plane
        blocks = half if k == 0 else plane
        count = blocks * most
        if partial and first == 0:
            gates_up[:, 0:count, :] = jnp.zeros((2, count, hidden), F32)

        @pl.loop(first, last)
        def _(q):
            with jax.named_scope(f"wait_came{k}"):
                if k == 0:
                    block_copy(came, 1, half, q, s_back.at[k], r_came.at[k, q]).wait_recv()
                else:
                    @pl.when(inner)
                    def _():
                        block_copy(came, base + 1, base + plane, q, s_back.at[k], r_came.at[k, q]).wait_recv()

                    @pl.when(jnp.logical_not(inner))
                    def _():
                        block_copy(came, base, base + plane, q, s_back.at[k], r_came.at[k, q]).wait_recv()

            if after is not None:
                after(q)

            def group(g):
                block = came[pl.ds(base + g * unit, unit), quad_rows(q), :].reshape(rows, piece)
                for j in range(unit):
                    at = slice(j * piece, (j + 1) * piece) if partial else columns(q, j)
                    x[pl.ds(g * part, part), at] = jnp.dot(
                        gather[j], block, preferred_element_type=F32).astype(BF16)

            with jax.named_scope(f"unpack{k}"):
                groups(blocks // unit, group)

            if partial:
                with jax.named_scope(f"gate_up{k}"):
                    for t in range(tiles):
                        for i, w in enumerate((wg, wu)):
                            gates_up[i, 0:count, t * step:(t + 1) * step] += jnp.dot(
                                x[0:count, 0:wide_cols], w[quad_columns(q), t * step:(t + 1) * step],
                                preferred_element_type=F32)

    def activate(k, h, partial=False):
        count = (half if k == 0 else plane) * most

        @pl.loop(0, tiles)
        def _(t):
            with jax.named_scope(f"activate{k}"):
                if partial:
                    gate, up = gates_up[0, 0:count, tile(t)], gates_up[1, 0:count, tile(t)]
                else:
                    gate = jnp.dot(x[0:count, :], wg[:, tile(t)], preferred_element_type=F32)
                    up = jnp.dot(x[0:count, :], wu[:, tile(t)], preferred_element_type=F32)
                h[0:count, tile(t)] = (gate / (1.0 + jnp.exp(-gate)) * up).astype(BF16)

    def down_quad(k, h, q, edge=False):
        base = 0 if k == 0 else half + (k - 1) * plane
        blocks = half if k == 0 else plane
        count = blocks * most

        with jax.named_scope(f"down{k}"):
            for j in range(unit):
                x[0:count, j * piece:(j + 1) * piece] = jnp.dot(
                    h[0:count, :], wd[:, columns(q, j)], preferred_element_type=F32).astype(BF16)

        def group(g):
            acc = jnp.zeros((rows, piece), F32)
            for j in range(unit):
                acc = acc + jnp.dot(spread[j], x[pl.ds(g * part, part), j * piece:(j + 1) * piece],
                                    preferred_element_type=F32)
            back[pl.ds(base + g * unit, unit), quad_rows(q), :] = acc.astype(BF16).reshape(unit, part, piece)

        with jax.named_scope(f"spread{k}"):
            groups(blocks // unit, group)

        if k == 0:
            def answer(off):
                remote(back.at[off, quad_rows(q), :], home.at[off, quad_rows(q), :],
                       s_back.at[k], r_home.at[k, q], off).start()

            each(1, plane if edge else half, answer)
            if edge:
                aside(back, hop_back, 1, q, plane, s_back.at[0])
                each(plane + 1, half, lambda off: aside(back, hop_back, 1, q, off, s_back.at[0]))
            home[0, quad_rows(q), :] = back[0, quad_rows(q), :]
        else:
            def reply(low):
                off = low + (1 - is_inner) * plane
                remote(back.at[base + low, quad_rows(q), :], home.at[k * half + off, quad_rows(q), :],
                       s_back.at[k], r_home.at[k, q], low, facing).start()

            @pl.when(jnp.logical_not(inner))
            def _():
                reply(0)

            each(1, plane, reply)

            @pl.when(inner)
            def _():
                home[k * half, quad_rows(q), :] = back[base, quad_rows(q), :]

    def down(k, h, edge=False):
        @pl.loop(0, quads)
        def _(q):
            down_quad(k, h, q, edge)

    def rooms():
        @pl.when(inner)
        def _():
            counted(half - 1 + 2 * (plane - 1), s_cnt, r_cnt).wait_recv()

        @pl.when(jnp.logical_not(inner))
        def _():
            counted(half - 1 + 2 * plane, s_cnt, r_cnt).wait_recv()

        sources = (me, flip(me, 3 * plane, bits), flip(me, 2 * plane, bits))

        def earlier(off, sums):
            peer = sum((1 << b) - v if (off >> b) % 2 else v for b, v in enumerate(mine)) if isinstance(
                off, int) else flip(me, off, bits)
            return tuple(t + seen[off] * jnp.where(peer < source, 1.0, 0.0) for t, source in zip(sums, sources))

        sums = tuple(jnp.zeros((1, lanes), F32) for _ in sources)
        if n <= 32:
            for off in range(n):
                sums = earlier(off, sums)
        else:
            sums = lax.fori_loop(0, n, earlier, sums)
        for k, taken in enumerate(sums):
            left[k] = jnp.broadcast_to(jnp.clip(limit - taken, 0.0, float(most)), (8, lanes))

    def combine(k, q):
        slots = [meta[k, c:c + 1, :] for c in (0, 1)]
        shares = [meta[k, c:c + 1, :] for c in (2, 3)]
        room_of = left[k].astype(BF16)
        eye = jnp.where(
            lax.broadcasted_iota(jnp.int32, (tok_rows, tok_rows), 0)
            == lax.broadcasted_iota(jnp.int32, (tok_rows, tok_rows), 1), 1.0, 0.0).astype(BF16)
        with jax.named_scope(f"wait_home{k}"):
            block_copy(home, k * half + 1, (k + 1) * half, q, s_back.at[k], r_home.at[k, q]).wait_recv()
        total[...] = jnp.zeros_like(total)

        def group(g):
            mine = code[...] + jnp.asarray(g * part, F32)
            weight = (jnp.where(mine == slots[0], shares[0], 0.0)
                      + jnp.where(mine == slots[1], shares[1], 0.0)).astype(BF16)
            weight = lax.dot_general(eye, weight, NT, preferred_element_type=F32)
            owner = lax.broadcasted_iota(jnp.int32, (lanes, rows), 0)
            pick = jnp.where(owner == ((lane[0:1, :] + g * unit) ^ me), 1.0, 0.0).astype(BF16)
            room = jnp.dot(room_of, pick, preferred_element_type=F32)[0:1, :]
            weight = jnp.where(room > lane[2:3, :].astype(F32), weight, 0.0)
            block = home[pl.ds(k * half + g * unit, unit), quad_rows(q), :].reshape(rows, piece)
            for j in range(unit):
                masked = jnp.where(lane[1:2, :] == j, weight, 0.0).astype(BF16)
                total[:, j * piece:(j + 1) * piece] += jnp.dot(masked, block, preferred_element_type=F32)

        with jax.named_scope(f"combine{k}"):
            groups(half // unit, group)

    def combine_far(k, q):
        combine(k, q)
        at = quad_columns(q)
        mixed[k - 1, :, at] = total[...].astype(BF16)
        into, arrived = (cross, r_cross) if k == 1 else (stage, r_stage)
        remote(mixed.at[k - 1, :, at], into.at[:, at], s_mixed.at[k - 1], arrived.at[q], 3 * plane).start()

    def forward(q):
        at = quad_columns(q)
        with jax.named_scope("wait_stage"):
            remote(stage.at[:, at], stage.at[:, at], s_stage, r_stage.at[q], relay_off).wait_recv()
        remote(stage.at[:, at], cross.at[:, at], s_stage, r_cross.at[q], plane).start()

    def pack_own(first, last, edge=False):
        @pl.loop(first, last)
        def _(q):
            pack(0, q, edge)

    def note_wait(k):
        with jax.named_scope("note"):
            remote(note, meta.at[k], s_note, r_note.at[k - 1], relay_off).wait_recv()

    def relay_in(k, first, last):
        @pl.loop(first, last)
        def _(q):
            pack_far(k, q)

    @pl.when(jnp.logical_not(inner))
    def _():
        send_far()

    early = max(1, quads // 4)
    late = max(early, quads - 1)

    def loaded():
        for load in loads:
            load.wait()

    @pl.when(jnp.logical_not(inner))
    def _():
        pack_own(0, quads, True)
        loaded()

        def hop_on(q):
            pass_on(hop, came, 0, r_came, q)

        def hop_early(q):
            @pl.when(q < quads - 1)
            def _():
                hop_on(q)

        receive(2, after=hop_early, partial=True)
        activate(2, h, True)

        @pl.loop(0, quads)
        def _(q):
            down_quad(2, h, q)

            @pl.when(q == 0)
            def _():
                hop_on(quads - 1)


    @pl.when(inner)
    def _():
        pack_own(0, quads // 2)
        send_far()
        note_wait(2)
        pass_counts(2)
        relay_in(2, 0, quads)
        pack_own(quads // 2, quads)
        loaded()
        note_wait(1)
        relay_in(1, 0, early)
        pass_counts(1)
        receive(2)
        activate(2, h)
        down(2, h)
        relay_in(1, early, late)

    def receive_one(first, last, after=None):
        receive(1, first, last, after, partial=True)

    def expert_one(first=0, after=None):
        receive_one(first, quads, after)
        activate(1, h, True)
        down(1, h)

    def own_down(q):
        down_quad(0, h_own, q)

    @pl.when(inner)
    def _():
        with jax.named_scope("rooms"):
            rooms()
        second, first = functools.partial(combine_far, 2), functools.partial(combine_far, 1)
        if quads == 4:
            steps = [(receive, 0, 0, 3), (second, 0), (relay_in, 1, 3, 4), (receive, 0, 3, 4), (activate, 0, h_own),
                     (second, 1), (own_down, 0), (own_down, 1), (receive_one, 0, 2), (second, 2),
                     (forward, 0), (receive_one, 2, 3), (second, 3), (expert_one, 3), (forward, 1), (own_down, 2),
                     (own_down, 3), (forward, 2), (first, 0), (first, 1), (forward, 3), (first, 2), (first, 3)]
        else:
            steps = [(relay_in, 1, late, quads), (receive, 0), (activate, 0, h_own)]
            steps += [(f, q) for f in (second, own_down) for q in range(quads)] + [(expert_one,)]
            steps += [(f, q) for f in (forward, first) for q in range(quads)]
        for act, *args in steps:
            act(*args)

    @pl.when(jnp.logical_not(inner))
    def _():
        receive(0)
        activate(0, h_own)
        down(0, h_own, True)

        def hop_back_on(q):
            pass_on(hop_back, home, 1, r_home, q)

        def first_back(q):
            @pl.when(q == quads - 2)
            def _():
                hop_back_on(0)

        expert_one(after=first_back)
        pl.loop(min(1, quads - 1), quads)(hop_back_on)
        with jax.named_scope("rooms"):
            rooms()

    @pl.loop(0, quads)
    def _(q):
        combine(0, q)
        at = quad_columns(q)
        with jax.named_scope("wait_cross"):
            remote(cross.at[:, at], cross.at[:, at], s_far, r_cross.at[q], relay_off).wait_recv()
        out[:, at] = (total[...] + cross[:, at].astype(F32)).astype(BF16)

    note_copy.wait_send()
    counted(half, s_cnt, r_cnt).wait_send()
    remote(tok, cross, s_far, r_far.at[0, 0], relay_off).wait_send()

    def sent_all(ref, first, last, send):
        some = ref.at[pl.ds(first, last - first)]
        remote(some, some, send, r_cnt, relay_off).wait_send()

    @pl.when(inner)
    def _():
        sent_all(sent, 1, half, s_sent.at[0])
        sent_all(back, 1, half, s_back.at[0])
        for k in (1, 2):
            base = half + (k - 1) * plane
            sent_all(sent, k * half + 1, (k + 1) * half, s_sent.at[k])
            sent_all(back, base + 1, base + plane, s_back.at[k])
            remote(mixed.at[k - 1], cross, s_mixed.at[k - 1], r_cnt, relay_off).wait_send()
        remote(stage, cross, s_stage, r_cnt, relay_off).wait_send()
        counted(2 * (half - 1), s_pass, r_cnt).wait_send()

    @pl.when(jnp.logical_not(inner))
    def _():
        for ref, send in ((sent, s_sent.at[0]), (back, s_back.at[0])):
            sent_all(ref, 1, plane, send)
            sent_all(ref, plane + 1, half, send)
        sent_all(hop, 0, plane, s_hop.at[0])
        sent_all(hop_back, 0, plane, s_hop.at[1])
        for k in (1, 2):
            base = half + (k - 1) * plane
            sent_all(back, base, base + plane, s_back.at[k])


def on_device(n, narrow, tokens, expert_ids, gate_values, capacity, w_gate, w_up, w_down):
    experts = capacity.shape[0]
    tok_rows, width = tokens.shape
    hidden = w_gate.shape[2]
    most = 3 * tok_rows // experts
    unit = 16 // math.gcd(16, most)
    half, plane = n // 2, n // PLANES
    rows = unit * unit * most
    quads = PIECES // unit
    lanes = -(-experts // 128) * 128

    i, j, r = np.meshgrid(np.arange(unit), np.arange(unit), np.arange(most), indexing="ij")
    i, j, r = i.reshape(-1), j.reshape(-1), r.reshape(-1)
    code = jnp.asarray(np.broadcast_to((i * most + r)[:, None], (rows, tok_rows)), F32)
    turn = jnp.asarray(np.broadcast_to(j[:, None], (rows, tok_rows)), F32)
    lane = jnp.asarray(np.stack([i, j, r] + [0 * r] * 5), jnp.int32)
    short = np.arange(unit * most)
    every = np.arange(unit)
    gather = (short[None, :, None] == (i * most + r)[None, None, :]) & (j[None] == every[:, None])[:, None, :]
    gather, spread = jnp.asarray(gather, BF16), jnp.asarray(gather.transpose(0, 2, 1), BF16)

    operands = [
        pltpu.with_memory_space_constraint(a, pltpu.HBM)
        for a in (expert_ids.T, gate_values.T, capacity[None], tokens, lane, code, turn, gather, spread,
                  w_gate, w_up, w_down)
    ]
    block = (PIECES * most, width // PIECES)
    vmem = pl.BlockSpec(memory_space=pltpu.VMEM)
    hbm = pl.BlockSpec(memory_space=pltpu.HBM)
    dma = pltpu.SemaphoreType.DMA
    return pl.pallas_call(
        functools.partial(kernel, n, narrow, most, unit),
        out_shape=jax.ShapeDtypeStruct((tok_rows, width), BF16),
        in_specs=[hbm] * 12,
        out_specs=vmem,
        scratch_shapes=[
            pltpu.VMEM((2, tok_rows), jnp.int32),
            pltpu.VMEM((2, tok_rows), BF16),
            pltpu.VMEM((1, experts), jnp.int32),
            pltpu.VMEM((tok_rows, width), BF16),
            pltpu.VMEM((8, rows), jnp.int32),
            pltpu.VMEM((rows, tok_rows), F32),
            pltpu.VMEM((rows, tok_rows), F32),
            pltpu.VMEM((unit, unit * most, rows), BF16),
            pltpu.VMEM((unit, rows, unit * most), BF16),
            pltpu.VMEM((width, hidden), BF16),
            pltpu.VMEM((width, hidden), BF16),
            pltpu.VMEM((hidden, width), BF16),
            pltpu.VMEM((3 * half,) + block, BF16),
            pltpu.VMEM((half + 2 * plane,) + block, BF16),
            pltpu.VMEM((half + 2 * plane,) + block, BF16),
            pltpu.VMEM((3 * half,) + block, BF16),
            pltpu.VMEM((plane,) + block, BF16),
            pltpu.VMEM((plane,) + block, BF16),
            pltpu.VMEM((2, tok_rows, width), BF16),
            pltpu.VMEM((2, tok_rows, width), BF16),
            pltpu.VMEM((tok_rows, width), BF16),
            pltpu.VMEM((tok_rows, width), BF16),
            pltpu.VMEM((half * most, width), BF16),
            pltpu.VMEM((2, half * most, hidden), F32),
            pltpu.VMEM((half * most, hidden), BF16),
            pltpu.VMEM((half * most, hidden), BF16),
            pltpu.VMEM((tok_rows, unit * width // PIECES), F32),
            pltpu.VMEM((8, tok_rows), F32),
            pltpu.VMEM((3, 8, tok_rows), F32),
            pltpu.VMEM((1, lanes), F32),
            pltpu.VMEM((n, 1, lanes), F32),
            pltpu.VMEM((3, 8, lanes), F32),
            dma((3,)), dma((3, quads)), dma((3,)), dma((3, quads)), dma, dma((2, quads)), dma((2,)),
            dma((quads,)), dma, dma((quads,)), dma((2,)), dma((2, quads)), dma, dma((2,)), dma, dma, dma, dma((2,)), dma((9,)), dma((3,)),
        ],
        compiler_params=pltpu.CompilerParams(
            collective_id=0, has_side_effects=True, vmem_limit_bytes=(52 if quads > 1 else 60) * 1024 * 1024
        ),
    )(*operands)


def solution(mesh):
    both = ("wide", "narrow")
    n, narrow = mesh.shape["wide"] * mesh.shape["narrow"], mesh.shape["narrow"]
    return jax.shard_map(
        functools.partial(on_device, n, narrow),
        mesh=mesh,
        in_specs=(P(both, None), P(both, None), P(both, None), P(),
                  P(both, None, None), P(both, None, None), P(both, None, None)),
        out_specs=P(both, None),
        check_vma=False,
    )
```
